8 devices in a mesh: replica: 1 (over z), yz: 2 (over y), x: 4 (over x, core).
Axes of the slice: x: 2, y: 2, z: 1, core: 2. Of those that a mesh axis runs over, the one named last changes fastest.
Arguments:
- hidden: bfloat16 [512, 4096], P('replica', ('x', 'yz'))
- seq_lens: int32 [512], P(('replica', 'yz', 'x'))
- attn_gain: bfloat16 [1, 4096], replicated
- mlp_gain: bfloat16 [1, 4096], replicated
- w_qkv: bfloat16 [1, 4096, 4352], P(None, None, 'yz')
- w_out: bfloat16 [1, 4096, 4096], P(None, 'yz')
- w_gate_up: bfloat16 [1, 4096, 2, 14336], P(None, None, None, 'yz')
- w_down: bfloat16 [1, 14336, 4096], P(None, 'yz')
- k_cache: bfloat16 [1, 512, 2048, 128], P(None, ('replica', 'yz', 'x'))
- v_cache: bfloat16 [1, 512, 2048, 128], P(None, ('replica', 'yz', 'x'))
Outputs:
- output 1: bfloat16 [512, 4096], P('replica', ('x', 'yz'))
- output 2: bfloat16 [1, 512, 2048, 128], P(None, ('replica', 'yz', 'x'))
- output 3: bfloat16 [1, 512, 2048, 128], P(None, ('replica', 'yz', 'x'))
All inputs are finite; a program needn't handle non-finite values.
Results may differ from the reference program's by a relative error of at most 0.0136421.
Values are sent between devices in bfloat16 or wider.
A program may use at most 1.5 GiB of HBM per device.

```python
import jax
import jax.numpy as jnp
from jax import lax

MODEL_DIM = 4096
Q_HEADS = 32
HEAD_DIM = 128
FFN_DIM = 14336
LAYERS = 1
SEQ_LEN = 2048
PART_BATCH = 512
BLOCK_ROWS = 8
ATTN_WIDTH = Q_HEADS * HEAD_DIM
QKV_WIDTH = ATTN_WIDTH + 2 * HEAD_DIM
NORM_EPS = 1e-5


def setup_inputs(seed: int = 0, part: int = 0) -> dict:
    root_key = jax.random.key(seed)
    shared = jax.random.split(root_key, 6)
    own_keys = jax.random.split(jax.random.fold_in(root_key, part), 6)
    cache_shape = (LAYERS, PART_BATCH, SEQ_LEN, HEAD_DIM)
    profile = 0.3 + 1.7 * jnp.arange(MODEL_DIM, dtype=jnp.float32) / MODEL_DIM
    row_scale = jnp.exp(0.5 * jax.random.normal(own_keys[0], (PART_BATCH, 1), jnp.float32))
    hidden = jax.random.normal(own_keys[1], (PART_BATCH, MODEL_DIM), jnp.float32) * profile * row_scale
    seq_lens = jax.random.randint(own_keys[2], (PART_BATCH,), 1, SEQ_LEN, dtype=jnp.int32)
    seq_lens = seq_lens.at[0].set(SEQ_LEN - 1).at[1].set(1)
    attn_gain = 1.0 + 0.5 * jax.random.normal(shared[0], (LAYERS, MODEL_DIM), jnp.float32)
    mlp_gain = 1.0 + 0.5 * jax.random.normal(shared[1], (LAYERS, MODEL_DIM), jnp.float32)
    w_qkv = jax.random.normal(shared[2], (LAYERS, MODEL_DIM, QKV_WIDTH), jnp.float32) * MODEL_DIM ** -0.5
    w_out = jax.random.normal(shared[3], (LAYERS, ATTN_WIDTH, MODEL_DIM), jnp.float32) * ATTN_WIDTH ** -0.5
    w_gate_up = jax.random.normal(shared[4], (LAYERS, MODEL_DIM, 2, FFN_DIM), jnp.float32) * MODEL_DIM ** -0.5
    w_down = jax.random.normal(shared[5], (LAYERS, FFN_DIM, MODEL_DIM), jnp.float32) * FFN_DIM ** -0.5
    k_cache = 2.0 * jax.random.normal(own_keys[3], cache_shape, jnp.float32)
    rand_walk = jnp.cumsum(jax.random.normal(own_keys[4], cache_shape, jnp.float32), axis=2)
    v_cache = rand_walk * (2.0 / SEQ_LEN ** 0.5) + jax.random.normal(own_keys[5], cache_shape, jnp.float32)
    return {
        'hidden': hidden.astype(jnp.bfloat16),
        'seq_lens': seq_lens,
        'attn_gain': attn_gain.astype(jnp.bfloat16),
        'mlp_gain': mlp_gain.astype(jnp.bfloat16),
        'w_qkv': w_qkv.astype(jnp.bfloat16),
        'w_out': w_out.astype(jnp.bfloat16),
        'w_gate_up': w_gate_up.astype(jnp.bfloat16),
        'w_down': w_down.astype(jnp.bfloat16),
        'k_cache': k_cache.astype(jnp.bfloat16),
        'v_cache': v_cache.astype(jnp.bfloat16),
    }


def rms_bf16(hid_state, gain):
    hid_f = hid_state.astype(jnp.float32)
    inv_scale = lax.rsqrt(jnp.mean(hid_f * hid_f, axis=-1, keepdims=True) + NORM_EPS)
    return (hid_f * inv_scale * gain.astype(jnp.float32)).astype(jnp.bfloat16)


def attend_block(row_block):
    z_rows, k_layer, v_layer, lens_blk = row_block
    queries = z_rows[:, :ATTN_WIDTH].reshape(BLOCK_ROWS, Q_HEADS, HEAD_DIM)
    k_new = z_rows[:, ATTN_WIDTH:ATTN_WIDTH + HEAD_DIM]
    v_new = z_rows[:, ATTN_WIDTH + HEAD_DIM:]
    slot_ids = jnp.arange(SEQ_LEN)
    at_slot = (slot_ids[None, :] == lens_blk[:, None])[:, :, None]
    k_upd = jnp.where(at_slot, k_new[:, None, :], k_layer)
    v_upd = jnp.where(at_slot, v_new[:, None, :], v_layer)
    scores = jnp.einsum('bhd,bsd->bhs', queries.astype(jnp.float32), k_upd.astype(jnp.float32)) * HEAD_DIM ** -0.5
    visible = (slot_ids[None, :] <= lens_blk[:, None])[:, None, :]
    scores = jnp.where(visible, scores, -1e30)
    probs_bf = jax.nn.softmax(scores, axis=-1).astype(jnp.bfloat16)
    outputs = jnp.einsum('bhs,bsd->bhd', probs_bf.astype(jnp.float32), v_upd.astype(jnp.float32)).astype(jnp.bfloat16)
    return outputs.reshape(BLOCK_ROWS, ATTN_WIDTH), k_upd, v_upd


def reference(hidden, seq_lens, attn_gain, mlp_gain, w_qkv, w_out, w_gate_up, w_down, k_cache, v_cache):
    num_blocks = PART_BATCH // BLOCK_ROWS

    def layer_step(hid_state, per_layer):
        gain_attn, gain_mlp, layer_qkv, layer_out, layer_gu, layer_down, k_layer, v_layer = per_layer
        normed = rms_bf16(hid_state, gain_attn)
        z_rows = jnp.dot(normed, layer_qkv, preferred_element_type=jnp.float32).astype(jnp.bfloat16)
        attn_out, k_upd, v_upd = lax.map(attend_block, (
            z_rows.reshape(num_blocks, BLOCK_ROWS, QKV_WIDTH),
            k_layer.reshape(num_blocks, BLOCK_ROWS, SEQ_LEN, HEAD_DIM),
            v_layer.reshape(num_blocks, BLOCK_ROWS, SEQ_LEN, HEAD_DIM),
            seq_lens.reshape(num_blocks, BLOCK_ROWS)))
        attn_out = attn_out.reshape(PART_BATCH, ATTN_WIDTH)
        hid_state = (hid_state.astype(jnp.float32) + jnp.dot(attn_out, layer_out, preferred_element_type=jnp.float32)).astype(jnp.bfloat16)
        normed = rms_bf16(hid_state, gain_mlp)
        gate_up = jnp.dot(normed, layer_gu.reshape(MODEL_DIM, 2 * FFN_DIM), preferred_element_type=jnp.float32).astype(jnp.bfloat16)
        gate_val = gate_up[:, :FFN_DIM].astype(jnp.float32)
        up_val = gate_up[:, FFN_DIM:].astype(jnp.float32)
        mlp_mixed = (jax.nn.silu(gate_val) * up_val).astype(jnp.bfloat16)
        hid_state = (hid_state.astype(jnp.float32) + jnp.dot(mlp_mixed, layer_down, preferred_element_type=jnp.float32)).astype(jnp.bfloat16)
        return hid_state, (k_upd.reshape(PART_BATCH, SEQ_LEN, HEAD_DIM), v_upd.reshape(PART_BATCH, SEQ_LEN, HEAD_DIM))

    hidden_out, caches = lax.scan(layer_step, hidden, (attn_gain, mlp_gain, w_qkv, w_out, w_gate_up, w_down, k_cache, v_cache))
    return hidden_out, caches[0], caches[1]
```

```python
import functools

import jax
import jax.numpy as jnp
from jax import lax
from jax.experimental import pallas as pl
from jax.experimental.pallas import tpu as pltpu
from jax.sharding import PartitionSpec as P

NORM_EPS = 1e-5
MESH = pl.DeviceIdType.MESH
MIB = 1 << 20
VMEM = pltpu.VMEM
DMA = pltpu.SemaphoreType.DMA


def place():
    yz = lax.axis_index('yz')
    x = lax.axis_index('x')
    return yz, x // 2, x % 2


def device(yz, chip, core):
    return {'yz': yz, 'x': 2 * chip + core}


def remote(src, dst, send, recv, target):
    return pltpu.make_async_remote_copy(src_ref=src, dst_ref=dst, send_sem=send, recv_sem=recv,
                                        device_id=target, device_id_type=MESH)


def greet(peers):
    barrier = pltpu.get_barrier_semaphore()
    for peer in peers:
        pl.semaphore_signal(barrier, inc=1, device_id=peer, device_id_type=MESH)
    pl.semaphore_wait(barrier, len(peers))


def lanes(start, size, unit=128):
    return pl.ds(pl.multiple_of(start, unit), size)


def dot(a, b):
    return jnp.dot(a, b, preferred_element_type=jnp.float32)


def qkv_kernel(h_ref, gain_ref, w_ref, z_ref, hx_ref, wbuf, ubuf, zbuf, w_sem, send, recv, zsend, zrecv):
    yz, chip, core = place()
    cols = h_ref.shape[-1]
    width = z_ref.shape[-1]
    parts = ((0, 512), (512, width - 512))
    step = w_ref.shape[1] - width
    model = hx_ref.shape[-1]
    loads = []
    for n, (off, size) in enumerate(parts):
        loads.append(pltpu.make_async_copy(w_ref.at[:, lanes(core * step + off, size)],
                                           wbuf.at[:, pl.ds(off, size)], w_sem.at[n]))
        loads[-1].start()
    ynbr, xnbr = device(1 - yz, chip, core), device(yz, 1 - chip, core)
    diag, partner = device(1 - yz, 1 - chip, core), device(yz, chip, 1 - core)
    far = device(1 - yz, chip, 1 - core)
    greet((ynbr, xnbr, diag, partner, far))

    def block(y, ch, co):
        return hx_ref.at[:, :, lanes((2 * (2 * ch + co) + y) * cols, cols, 512)]

    mine = block(yz, chip, core)
    copies = []
    for k, (src, target) in enumerate(((1 - chip, diag), (chip, ynbr), (1 - chip, xnbr), (chip, partner))):
        copies.append(remote(h_ref.at[:, src], mine, send.at[k], recv.at[k], target))
        copies[-1].start()
    hx_ref[:, :, lanes((2 * (2 * chip + core) + yz) * cols, cols, 512)] = h_ref[:, chip]
    arrivals = ((1, block(1 - yz, chip, core)), (2, block(yz, 1 - chip, core)), (0, block(1 - yz, 1 - chip, core)))
    for k, (which, ref) in enumerate(arrivals):
        copies[which].wait_recv()
        copies.append(remote(ref, ref, send.at[4 + k], recv.at[4 + k], partner))
        copies[-1].start()
    for k in (3, 4, 5, 6):
        copies[k].wait_recv()

    gain = gain_ref[...].astype(jnp.float32)
    chunk = 32
    for half in range(2):
        @pl.loop(0, 128 // chunk)
        def _(r):
            hid = hx_ref[half, lanes(r * chunk, chunk, chunk), :].astype(jnp.float32)
            inv = lax.rsqrt(jnp.sum(hid * hid, axis=1, keepdims=True) / model + NORM_EPS)
            ubuf[lanes(half * 128 + r * chunk, chunk, chunk), :] = (hid * inv * gain).astype(jnp.bfloat16)

    slot = 2 * yz + core
    zcopies = []
    for n, (off, size) in enumerate(parts):
        loads[n].wait()
        z = dot(ubuf[...], wbuf[:, off:off + size]).astype(jnp.bfloat16)
        zbuf[:, :, off:off + size] = z.reshape(4, 64, size)
        for k, (y, co, target) in enumerate(((1 - yz, core, ynbr), (1 - yz, 1 - core, far), (yz, 1 - core, partner))):
            zcopies.append(remote(zbuf.at[2 * y + co, :, pl.ds(off, size)], z_ref.at[slot, :, pl.ds(off, size)],
                                  zsend.at[n, k], zrecv.at[n, k], target))
            zcopies[-1].start()
    z_ref[slot] = zbuf[slot]
    for copy in copies:
        copy.wait_send()
    for copy in zcopies:
        copy.wait()


def project_qkv(h, gain, w_qkv):
    model, half = w_qkv.shape
    width = (half // 128 + 1) // 2 * 128
    h4 = h.reshape(2, 2, 128, h.shape[1])
    return pl.pallas_call(
        qkv_kernel,
        out_shape=(jax.ShapeDtypeStruct((4, 64, width), jnp.bfloat16),
                   jax.ShapeDtypeStruct((2, 128, model), jnp.bfloat16)),
        in_specs=[pl.BlockSpec(memory_space=VMEM), pl.BlockSpec(memory_space=VMEM), pl.BlockSpec(memory_space=pl.ANY)],
        out_specs=(pl.BlockSpec(memory_space=VMEM), pl.BlockSpec(memory_space=VMEM)),
        scratch_shapes=[VMEM((model, width), jnp.bfloat16), VMEM((256, model), jnp.bfloat16),
                        VMEM((4, 64, width), jnp.bfloat16), DMA((2,)), DMA((7,)), DMA((7,)), DMA((2, 3)), DMA((2, 3))],
        compiler_params=pltpu.CompilerParams(collective_id=0, has_side_effects=True, vmem_limit_bytes=40 * MIB),
        name='qkv',
    )(h4, gain, w_qkv)


def attention_kernel(lens_ref, z_ref, k_ref, v_ref, o_ref, ko_ref, vo_ref, qs, kn, vn, os, kbuf, vbuf, isem, osem, *,
                     heads, slots, ahead):
    seqs, length, dim = k_ref.shape
    tiles = (heads + 2) // 2
    split = tiles // 2

    def tile(t):
        y, local = t // tiles, t % tiles
        co = 1 if local >= split else 0
        first = (local - split * co) * dim
        return z_ref[2 * y + co, :, first:first + dim].astype(jnp.float32)

    def fetch(b):
        s = lax.rem(b, slots)
        return (pltpu.make_async_copy(k_ref.at[b], kbuf.at[s], isem.at[0, s]),
                pltpu.make_async_copy(v_ref.at[b], vbuf.at[s], isem.at[1, s]))

    def flush(b):
        s = lax.rem(b, slots)
        return (pltpu.make_async_copy(kbuf.at[s], ko_ref.at[b], osem.at[0, s]),
                pltpu.make_async_copy(vbuf.at[s], vo_ref.at[b], osem.at[1, s]))

    for b in range(ahead):
        for copy in fetch(jnp.int32(b)):
            copy.start()
    for t in range(heads):
        qs[pl.ds(t, seqs, stride=heads), :] = tile(t)
    kn[...] = tile(heads)
    vn[...] = tile(heads + 1)

    @pl.loop(0, seqs)
    def _(b):
        nxt = b + ahead

        @pl.when(nxt < seqs)
        def _():
            @pl.when(nxt >= slots)
            def _():
                for copy in flush(nxt - slots):
                    copy.wait()
            for copy in fetch(nxt):
                copy.start()

        s = lax.rem(b, slots)
        for copy in fetch(b):
            copy.wait()
        last = lens_ref[b]
        base = pl.multiple_of(last // 16 * 16, 16)
        row = lax.broadcasted_iota(jnp.int32, (16, dim), 0) == last - base
        for buf, new in ((kbuf, kn), (vbuf, vn)):
            old = buf[s, pl.ds(base, 16), :].astype(jnp.float32)
            buf[s, pl.ds(base, 16), :] = jnp.where(row, new[pl.ds(b, 1), :], old).astype(jnp.bfloat16)
        for copy in flush(b):
            copy.start()
        q = qs[lanes(b * heads, heads, heads), :].astype(jnp.bfloat16)
        scores = lax.dot_general(q, kbuf[s], (((1,), (1,)), ((), ())), preferred_element_type=jnp.float32) * dim ** -0.5
        seen = lax.broadcasted_iota(jnp.int32, (heads, length), 1) <= last
        scores = jnp.where(seen, scores, -1e30)
        probs = jnp.exp(scores - jnp.max(scores, axis=1, keepdims=True))
        probs = probs * (1.0 / jnp.sum(probs, axis=1, keepdims=True))
        os[lanes(b * heads, heads, heads), :] = dot(probs.astype(jnp.bfloat16), vbuf[s])

    for t in range(heads):
        o_ref[:, t * dim:(t + 1) * dim] = os[pl.ds(t, seqs, stride=heads), :].astype(jnp.bfloat16)

    @pl.loop(seqs - slots, seqs)
    def _(b):
        for copy in flush(b):
            copy.wait()


def attend(lens, z, k_cache, v_cache):
    seqs, length, dim = k_cache.shape
    heads = 32
    slots, ahead = 12, 6
    anywhere = pl.BlockSpec(memory_space=pl.ANY)
    vmem = pl.BlockSpec(memory_space=VMEM)
    return pl.pallas_call(
        functools.partial(attention_kernel, heads=heads, slots=slots, ahead=ahead),
        out_shape=(jax.ShapeDtypeStruct((seqs, heads * dim), jnp.bfloat16),
                   jax.ShapeDtypeStruct(k_cache.shape, k_cache.dtype),
                   jax.ShapeDtypeStruct(v_cache.shape, v_cache.dtype)),
        in_specs=[pl.BlockSpec(memory_space=pltpu.SMEM), vmem, anywhere, anywhere],
        out_specs=(vmem, anywhere, anywhere),
        scratch_shapes=[VMEM((seqs * heads, dim), jnp.float32), VMEM((seqs, dim), jnp.float32),
                        VMEM((seqs, dim), jnp.float32), VMEM((seqs * heads, dim), jnp.float32),
                        VMEM((slots, length, dim), jnp.bfloat16), VMEM((slots, length, dim), jnp.bfloat16),
                        DMA((2, slots)), DMA((2, slots))],
        compiler_params=pltpu.CompilerParams(vmem_limit_bytes=40 * MIB),
        name='attention',
    )(lens, z, k_cache, v_cache)


def mlp_kernel(o_ref, hx_ref, gain_ref, spread_ref, wo_ref, gu_ref, wd_ref, out_ref,
               og, hres, wo, ys, yr, h1, ubuf, ue, gub, mbuf, wd, ps, pr, acc, fs, fr, xs,
               s_wo, s_h, s_gu, s_wd, send, recv, ysend, yrecv, hsend, hrecv, psend, precv, fsend, frecv, xsend, xrecv):
    yz, chip, core = place()
    half = wo_ref.shape[0]
    model = wo_ref.shape[1]
    inner = gu_ref.shape[2] // 2
    ynbr, xnbr, partner = device(1 - yz, chip, core), device(yz, 1 - chip, core), device(yz, chip, 1 - core)

    wo_copies = [pltpu.make_async_copy(wo_ref.at[:, lanes(core * half + n * 512, 512, 512)], wo.at[n], s_wo.at[n])
                 for n in range(4)]
    h_copy = pltpu.make_async_copy(hx_ref.at[:, :, lanes(core * half, half, 512)], hres, s_h.at[0])

    def gu_copies(n):
        s = lax.rem(n, 2)
        return [pltpu.make_async_copy(gu_ref.at[pl.ds(r * 1024, 1024), :, lanes(core * inner + n * 512, 512, 512)],
                                      gub.at[s, pl.ds(r * 1024, 1024)], s_gu.at[s, r]) for r in range(4)]

    def column(t):
        k = t // 2
        y = jnp.where(k < 2, 1 - yz, yz)
        ch = jnp.where(k % 2 == 0, 1 - chip, chip)
        co = jnp.where(t % 2 == 0, 1 - core, core)
        return 2 * (2 * ch + co) + y

    def wd_copies(t):
        s = lax.rem(t, 3)
        rows = inner // 2
        return [pltpu.make_async_copy(wd_ref.at[lanes(core * inner + r * rows, rows, rows), lanes(column(t) * 512, 512, 512)],
                                      wd.at[s, pl.ds(r * rows, rows)], s_wd.at[s, r]) for r in range(2)]

    for copy in wo_copies:
        copy.start()
    h_copy.start()
    greet((ynbr, xnbr, partner))

    slot = 2 * yz + core
    to_y = remote(o_ref.at[:, lanes((1 - yz) * half, half, 512)], og.at[slot], send.at[0], recv.at[0], ynbr)
    to_y.start()
    to_p = remote(o_ref.at[:, lanes(yz * half, half, 512)], og.at[slot], send.at[1], recv.at[1], partner)
    to_p.start()
    og[slot] = o_ref[:, lanes(yz * half, half, 512)]
    for n in range(2):
        for copy in gu_copies(jnp.int32(n)):
            copy.start()
    for t in range(3):
        for copy in wd_copies(jnp.int32(t)):
            copy.start()
    to_y.wait_recv()
    theirs = og.at[2 * (1 - yz) + core]
    onward = remote(theirs, theirs, send.at[2], recv.at[2], partner)
    onward.start()
    to_p.wait_recv()
    onward.wait_recv()

    def y_copy(n):
        return remote(ys.at[n], yr.at[n], ysend.at[n], yrecv.at[n], ynbr)

    for copy in wo_copies:
        copy.wait()

    @pl.loop(0, 4)
    def _(n):
        ys[n] = dot(og[...].reshape(256, half), wo[n]).astype(jnp.bfloat16)
        y_copy(n).start()

    h_copy.wait()

    def h_send(n):
        return remote(h1.at[4 * core + n], h1.at[4 * core + n], hsend.at[n], hrecv.at[n], partner)

    @pl.loop(0, 4)
    def _(n):
        y_copy(n).wait_recv()
        total = ys[n].astype(jnp.float32) + yr[n].astype(jnp.float32)
        res = hres[:, :, lanes(n * 512, 512, 512)].reshape(256, 512).astype(jnp.float32)
        h1[4 * core + n] = (res + total).astype(jnp.bfloat16)
        h_send(n).start()

    @pl.loop(0, 4)
    def _(n):
        h_send(n).wait_recv()

    gain = gain_ref[...].astype(jnp.float32)

    @pl.loop(0, 8)
    def _(r):
        rows = lanes(r * 32, 32, 32)
        power = jnp.zeros((32, 1), jnp.float32)
        for n in range(8):
            hid = h1[n, rows, :].astype(jnp.float32)
            power += jnp.sum(hid * hid, axis=1, keepdims=True)
        inv = lax.rsqrt(power / model + NORM_EPS)
        for n in range(8):
            hid = h1[n, rows, :].astype(jnp.float32)
            ubuf[rows, n * 512:(n + 1) * 512] = (hid * inv * gain[:, n * 512:(n + 1) * 512]).astype(jnp.bfloat16)

    spread = spread_ref[...]

    @pl.loop(0, model // 512)
    def _(t):
        for q in range(4):
            wide = dot(ubuf[:, lanes(t * 512 + q * 128, 128)], spread).astype(jnp.bfloat16)
            ue[:256, lanes(t * 1024 + q * 256, 256, 256)] = wide[:, :256]
            ue[256:, lanes(t * 1024 + q * 256, 256, 256)] = wide[:, 256:]

    @pl.loop(0, inner // 512)
    def _(n):
        s = lax.rem(n, 2)
        for copy in gu_copies(n):
            copy.wait()
        both = dot(ue[...], gub.at[s].reshape(2 * model, 512)[...])

        @pl.when(n + 2 < inner // 512)
        def _():
            for copy in gu_copies(n + 2):
                copy.start()

        gate = both[:256].astype(jnp.bfloat16).astype(jnp.float32)
        up = both[256:].astype(jnp.bfloat16).astype(jnp.float32)
        mbuf[:, lanes(n * 512, 512, 512)] = (gate * jax.nn.sigmoid(gate) * up).astype(jnp.bfloat16)

    def p_copy(k):
        return remote(ps.at[k], pr.at[k], psend.at[k], precv.at[k], partner)

    def f_copy(k):
        return remote(fs.at[k], fr.at[k], fsend.at[k], frecv.at[k], ynbr)

    x_copy = remote(xs, out_ref.at[:, chip], xsend.at[0], xrecv.at[0], xnbr)

    @pl.loop(0, 4)
    def _(k):
        for side in range(2):
            t = 2 * k + side
            s = lax.rem(t, 3)
            for copy in wd_copies(t):
                copy.wait()
            part = dot(mbuf[...], wd[s])

            @pl.when(t + 3 < 8)
            def _():
                for copy in wd_copies(t + 3):
                    copy.start()

            if side == 0:
                ps[k] = part.astype(jnp.bfloat16)
                p_copy(k).start()
            else:
                acc[...] = part
        p_copy(k).wait_recv()
        acc[...] += pr[k].astype(jnp.float32)

        @pl.when(k < 2)
        def _():
            fs[k] = acc[...].astype(jnp.bfloat16)
            f_copy(k).start()

        @pl.when(k >= 2)
        def _():
            f_copy(k - 2).wait_recv()
            total = acc[...] + fr[k - 2].astype(jnp.float32)
            final = (h1[column(2 * k + 1)].astype(jnp.float32) + total).astype(jnp.bfloat16).reshape(2, 128, 512)

            @pl.when(k == 2)
            def _():
                xs[...] = final
                x_copy.start()

            @pl.when(k == 3)
            def _():
                out_ref[:, chip] = final

    x_copy.wait()
    for copy in (to_y, to_p, onward):
        copy.wait_send()

    @pl.loop(0, 4)
    def _(n):
        y_copy(n).wait_send()
        h_send(n).wait_send()
        p_copy(n).wait_send()

    @pl.loop(0, 2)
    def _(n):
        f_copy(n).wait_send()


def mlp(o, hx, gain, w_out, w_gate_up, w_down):
    half, model = w_out.shape
    inner = w_gate_up.shape[2] // 2
    anywhere = pl.BlockSpec(memory_space=pl.ANY)
    vmem = pl.BlockSpec(memory_space=VMEM)
    bf16 = jnp.bfloat16
    column = jnp.arange(512)[None, :]
    spread = (column % 256 == 2 * jnp.arange(128)[:, None] + column // 256).astype(bf16)
    out = pl.pallas_call(
        mlp_kernel,
        out_shape=jax.ShapeDtypeStruct((2, 2, 128, 512), bf16),
        in_specs=[vmem, anywhere, vmem, vmem, anywhere, anywhere, anywhere],
        out_specs=vmem,
        scratch_shapes=[
            VMEM((4, 64, half), bf16), VMEM((2, 128, half), bf16), VMEM((4, half, 512), bf16),
            VMEM((4, 256, 512), bf16), VMEM((4, 256, 512), bf16), VMEM((8, 256, 512), bf16),
            VMEM((256, model), bf16), VMEM((512, 2 * model), bf16), VMEM((2, model, 2, 512), bf16),
            VMEM((256, inner), bf16), VMEM((3, inner, 512), bf16),
            VMEM((4, 256, 512), bf16), VMEM((4, 256, 512), bf16), VMEM((256, 512), jnp.float32),
            VMEM((2, 256, 512), bf16), VMEM((2, 256, 512), bf16), VMEM((2, 128, 512), bf16),
            DMA((4,)), DMA((1,)), DMA((2, 4)), DMA((3, 2)),
            DMA((3,)), DMA((3,)), DMA((4,)), DMA((4,)), DMA((4,)), DMA((4,)), DMA((4,)), DMA((4,)),
            DMA((2,)), DMA((2,)), DMA((1,)), DMA((1,)),
        ],
        compiler_params=pltpu.CompilerParams(collective_id=1, has_side_effects=True, vmem_limit_bytes=67043328),
        name='mlp',
    )(o, hx, gain, spread, w_out, w_gate_up, w_down)
    return out.reshape(512, 512)


def solution(mesh):
    batch_axes = ('replica', 'yz', 'x')
    hidden_spec = P('replica', ('x', 'yz'))
    cache_spec = P(None, batch_axes, None, None)

    def local_step(hidden, seq_lens, attn_gain, mlp_gain, w_qkv, w_out, w_gate_up, w_down, k_cache, v_cache):
        k_layers = []
        v_layers = []
        for layer in range(w_qkv.shape[0]):
            z, hx = project_qkv(hidden, attn_gain[layer:layer + 1], w_qkv[layer])
            o, k_upd, v_upd = attend(seq_lens, z, k_cache[layer], v_cache[layer])
            k_layers.append(k_upd)
            v_layers.append(v_upd)
            hidden = mlp(o, hx, mlp_gain[layer:layer + 1], w_out[layer], w_gate_up[layer], w_down[layer])
        return hidden, jnp.stack(k_layers), jnp.stack(v_layers)

    return jax.shard_map(
        local_step,
        mesh=mesh,
        in_specs=(hidden_spec, P(batch_axes), P(None, None), P(None, None), P(None, None, 'yz'), P(None, 'yz', None),
                  P(None, None, None, 'yz'), P(None, 'yz', None), cache_spec, cache_spec),
        out_specs=(hidden_spec, cache_spec, cache_spec),
        check_vma=False)
```

```python
import functools

import jax
import jax.numpy as jnp
from jax import lax
from jax.experimental import pallas as pl
from jax.experimental.pallas import tpu as pltpu
from jax.sharding import PartitionSpec as P

NORM_EPS = 1e-5
MESH = pl.DeviceIdType.MESH
MIB = 1 << 20
GROUP, DEPTH = 4, 4
VMEM = pltpu.VMEM
DMA = pltpu.SemaphoreType.DMA


def place():
    yz = lax.axis_index('yz')
    x = lax.axis_index('x')
    return yz, x // 2, x % 2


def device(yz, chip, core):
    return {'yz': yz, 'x': 2 * chip + core}


def remote(src, dst, send, recv, target):
    return pltpu.make_async_remote_copy(src_ref=src, dst_ref=dst, send_sem=send, recv_sem=recv,
                                        device_id=target, device_id_type=MESH)


def greet(peers):
    barrier = pltpu.get_barrier_semaphore()
    for peer in peers:
        pl.semaphore_signal(barrier, inc=1, device_id=peer, device_id_type=MESH)
    pl.semaphore_wait(barrier, len(peers))


def lanes(start, size, unit=128):
    return pl.ds(pl.multiple_of(start, unit), size)


def slot_columns(yz, core):
    return core * 2048 + yz * 1024


def dot(a, b):
    return jnp.dot(a, b, preferred_element_type=jnp.float32)


def qkv_kernel(h_ref, gain_ref, w_ref, z_ref, hres_ref, hx_ref, wbuf, ubuf, zbuf, w_sem, send, recv, zsend, zrecv):
    yz, chip, core = place()
    cols = h_ref.shape[-1]
    width = z_ref.shape[-1]
    parts = ((0, 512), (512, width - 512))
    step = w_ref.shape[1] - width
    model = hx_ref.shape[-1]
    loads = []
    for n, (off, size) in enumerate(parts):
        loads.append(pltpu.make_async_copy(w_ref.at[:, lanes(core * step + off, size)],
                                           wbuf.at[:, pl.ds(off, size)], w_sem.at[n]))
        loads[-1].start()
    ynbr, xnbr = device(1 - yz, chip, core), device(yz, 1 - chip, core)
    diag, partner = device(1 - yz, 1 - chip, core), device(yz, chip, 1 - core)
    far = device(1 - yz, chip, 1 - core)
    greet((ynbr, xnbr, diag, partner, far))

    def block(y, ch, co):
        return hx_ref.at[:, :, lanes((2 * (2 * ch + co) + y) * cols, cols, 512)]

    mine = block(yz, chip, core)
    copies = []
    for k, (src, target) in enumerate(((1 - chip, diag), (chip, ynbr), (1 - chip, xnbr), (chip, partner))):
        copies.append(remote(h_ref.at[:, src], mine, send.at[k], recv.at[k], target))
        copies[-1].start()
    hx_ref[:, :, lanes((2 * (2 * chip + core) + yz) * cols, cols, 512)] = h_ref[:, chip]
    arrivals = ((1, block(1 - yz, chip, core)), (2, block(yz, 1 - chip, core)), (0, block(1 - yz, 1 - chip, core)))
    for k, (which, ref) in enumerate(arrivals):
        copies[which].wait_recv()
        copies.append(remote(ref, ref, send.at[4 + k], recv.at[4 + k], partner))
        copies[-1].start()
    for k in (3, 4, 5, 6):
        copies[k].wait_recv()

    gain = gain_ref[...].astype(jnp.float32)
    chunk = 32
    for half in range(2):
        @pl.loop(0, 128 // chunk)
        def _(r):
            hid = hx_ref[half, lanes(r * chunk, chunk, chunk), :].astype(jnp.float32)
            inv = lax.rsqrt(jnp.sum(hid * hid, axis=1, keepdims=True) / model + NORM_EPS)
            ubuf[lanes(half * 128 + r * chunk, chunk, chunk), :] = (hid * inv * gain).astype(jnp.bfloat16)

    slot = 2 * yz + core
    zcopies = []
    for n, (off, size) in enumerate(parts):
        loads[n].wait()
        z = dot(ubuf[...], wbuf[:, off:off + size]).astype(jnp.bfloat16)
        zbuf[:, :, off:off + size] = z.reshape(4, 64, size)
        for k, (y, co, target) in enumerate(((1 - yz, core, ynbr), (1 - yz, 1 - core, far), (yz, 1 - core, partner))):
            zcopies.append(remote(zbuf.at[2 * y + co, :, pl.ds(off, size)], z_ref.at[slot, :, pl.ds(off, size)],
                                  zsend.at[n, k], zrecv.at[n, k], target))
            zcopies[-1].start()
    z_ref[slot] = zbuf[slot]
    hres_ref[...] = hx_ref[:, :, lanes(slot_columns(yz, core), 1024, 512)]
    for copy in copies:
        copy.wait_send()
    for copy in zcopies:
        copy.wait()


def project_qkv(h, gain, w_qkv):
    model, half = w_qkv.shape
    width = (half // 128 + 1) // 2 * 128
    h4 = h.reshape(2, 2, 128, h.shape[1])
    return pl.pallas_call(
        qkv_kernel,
        out_shape=(jax.ShapeDtypeStruct((4, 64, width), jnp.bfloat16),
                   jax.ShapeDtypeStruct((2, 128, model // 4), jnp.bfloat16)),
        in_specs=[pl.BlockSpec(memory_space=VMEM), pl.BlockSpec(memory_space=VMEM), pl.BlockSpec(memory_space=pl.ANY)],
        out_specs=(pl.BlockSpec(memory_space=VMEM), pl.BlockSpec(memory_space=VMEM)),
        scratch_shapes=[VMEM((2, 128, model), jnp.bfloat16), VMEM((model, width), jnp.bfloat16), VMEM((256, model), jnp.bfloat16),
                        VMEM((4, 64, width), jnp.bfloat16), DMA((2,)), DMA((7,)), DMA((7,)), DMA((2, 3)), DMA((2, 3))],
        compiler_params=pltpu.CompilerParams(collective_id=0, has_side_effects=True, vmem_limit_bytes=40 * MIB),
        name='qkv',
    )(h4, gain, w_qkv)


def attention_kernel(lens_ref, order_ref, z_ref, k_ref, v_ref, o_ref, ko_ref, vo_ref,
                     qs, kn, vn, os, kbuf, vbuf, sem, fsem, *, heads, group, depth, unit):
    seqs, length, dim = k_ref.shape
    tiles = (heads + 2) // 2
    split = tiles // 2
    groups = seqs // group
    sizes = length // unit

    def tile(t):
        y, local = t // tiles, t % tiles
        co = 1 if local >= split else 0
        first = (local - split * co) * dim
        return z_ref[2 * y + co, :, first:first + dim].astype(jnp.float32)

    def by_size(g, act):
        need = lens_ref[order_ref[g * group]] // unit + 1
        for size in range(1, sizes + 1):
            @pl.when(need == size)
            def _():
                act(size * unit)

    def fetch(g, rows):
        out = []
        for m in range(group):
            b = order_ref[g * group + m]
            s = lax.rem(g, depth) * group + m
            out.append(pltpu.make_async_copy(k_ref.at[b, pl.ds(0, rows)], kbuf.at[s, pl.ds(0, rows)], sem.at[0, s]))
            out.append(pltpu.make_async_copy(v_ref.at[b, pl.ds(0, rows)], vbuf.at[s, pl.ds(0, rows)], sem.at[1, s]))
        return out

    def flush(g):
        out = []
        for m in range(group):
            b = order_ref[g * group + m]
            s = lax.rem(g, depth) * group + m
            out.append(pltpu.make_async_copy(kbuf.at[s], ko_ref.at[b], fsem.at[0, s]))
            out.append(pltpu.make_async_copy(vbuf.at[s], vo_ref.at[b], fsem.at[1, s]))
        return out

    def arrive(g, begin):
        for copy in fetch(g, length):
            if begin:
                copy.start()
            else:
                copy.wait()

    for g in range(2):
        arrive(jnp.int32(g), True)
    for t in range(heads):
        qs[pl.ds(t, seqs, stride=heads), :] = tile(t)
    kn[...] = tile(heads)
    vn[...] = tile(heads + 1)

    @pl.loop(0, groups)
    def _(g):
        @pl.when(g >= depth - 2)
        def _():
            for copy in flush(g - (depth - 2)):
                copy.wait()

        @pl.when(g + 2 < groups)
        def _():
            arrive(g + 2, True)

        arrive(g, False)
        for m in range(group):
            b = order_ref[g * group + m]
            s = lax.rem(g, depth) * group + m
            last = lens_ref[b]
            base = pl.multiple_of(last // 16 * 16, 16)
            row = lax.broadcasted_iota(jnp.int32, (16, dim), 0) == last - base
            for buf, new in ((kbuf, kn), (vbuf, vn)):
                old = buf[s, pl.ds(base, 16), :].astype(jnp.float32)
                buf[s, pl.ds(base, 16), :] = jnp.where(row, new[pl.ds(b, 1), :], old).astype(jnp.bfloat16)

        for copy in flush(g):
            copy.start()

        def act(rows):
            scores = []
            for m in range(group):
                b = order_ref[g * group + m]
                s = lax.rem(g, depth) * group + m
                q = qs[lanes(b * heads, heads, heads), :].astype(jnp.bfloat16)
                raw = lax.dot_general(q, kbuf[s, :rows], (((1,), (1,)), ((), ())), preferred_element_type=jnp.float32)
                seen = lax.broadcasted_iota(jnp.int32, (heads, rows), 1) <= lens_ref[b]
                scores.append(jnp.where(seen, raw * dim ** -0.5, -1e30))
            tops = [jnp.max(x, axis=1, keepdims=True) for x in scores]
            probs = [jnp.exp(x - top) for x, top in zip(scores, tops)]
            sums = [1.0 / jnp.sum(x, axis=1, keepdims=True) for x in probs]
            for m in range(group):
                b = order_ref[g * group + m]
                s = lax.rem(g, depth) * group + m
                os[lanes(b * heads, heads, heads), :] = dot((probs[m] * sums[m]).astype(jnp.bfloat16), vbuf[s, :rows])

        by_size(g, act)

    for t in range(heads):
        o_ref[:, t * dim:(t + 1) * dim] = os[pl.ds(t, seqs, stride=heads), :].astype(jnp.bfloat16)

    @pl.loop(groups - (depth - 2), groups)
    def _(g):
        for copy in flush(g):
            copy.wait()


def by_length(lens):
    ids = jnp.arange(lens.shape[0])
    ahead = (lens[None, :] > lens[:, None]) | ((lens[None, :] == lens[:, None]) & (ids[None, :] < ids[:, None]))
    rank = jnp.sum(ahead.astype(jnp.int32), axis=1)
    order = jnp.sum(jnp.where(rank[None, :] == ids[:, None], ids[None, :], 0), axis=1).astype(jnp.int32)
    return order


def attend(lens, order, z, k_cache, v_cache):
    seqs, length, dim = k_cache.shape
    heads = 32
    group, depth, unit = GROUP, DEPTH, 256
    anywhere = pl.BlockSpec(memory_space=pl.ANY)
    vmem = pl.BlockSpec(memory_space=VMEM)
    smem = pl.BlockSpec(memory_space=pltpu.SMEM)
    return pl.pallas_call(
        functools.partial(attention_kernel, heads=heads, group=group, depth=depth, unit=unit),
        out_shape=(jax.ShapeDtypeStruct((seqs, heads * dim), jnp.bfloat16),
                   jax.ShapeDtypeStruct(k_cache.shape, k_cache.dtype), jax.ShapeDtypeStruct(v_cache.shape, v_cache.dtype)),
        in_specs=[smem, smem, vmem, anywhere, anywhere],
        out_specs=(vmem, anywhere, anywhere),
        scratch_shapes=[VMEM((seqs * heads, dim), jnp.float32), VMEM((seqs, dim), jnp.float32),
                        VMEM((seqs, dim), jnp.float32), VMEM((seqs * heads, dim), jnp.float32),
                        VMEM((group * depth, length, dim), jnp.bfloat16), VMEM((group * depth, length, dim), jnp.bfloat16),
                        DMA((2, group * depth)), DMA((2, group * depth))],
        compiler_params=pltpu.CompilerParams(vmem_limit_bytes=50 * MIB),
        name='attention',
    )(lens, order, z, k_cache, v_cache)


def mlp_kernel(o_ref, hres, gain_ref, wo_ref, gu_ref, wd_ref, out_ref,
               og, wo, ys, yr, own, h1, inv_ref, ubuf, ue, gub, gacc, mbuf, wd, ps, pr, acc, fs, fr, xs, st,
               s_wo, s_gu, s_wd, send, recv, ysend, yrecv, hsend, hrecv, asend, arecv, osend, orecv, ssend, srecv,
               psend, precv, fsend, frecv, xsend, xrecv):
    yz, chip, core = place()
    half = wo_ref.shape[0]
    model = wo_ref.shape[1]
    inner = gu_ref.shape[2] // 2
    tiles = inner // 512
    ynbr, xnbr, partner = device(1 - yz, chip, core), device(yz, 1 - chip, core), device(yz, chip, 1 - core)
    far = device(1 - yz, chip, 1 - core)

    wo_copies = [pltpu.make_async_copy(wo_ref.at[:, lanes(core * half + n * 512, 512, 512)], wo.at[n], s_wo.at[n])
                 for n in range(4)]

    def place_of(p):
        y = jnp.where(p < 4, yz, 1 - yz)
        return (p % 4) // 2 * 4 + 2 * y + p % 2

    def gu_copies(q):
        s = lax.rem(q, 3)
        n = lax.rem(q, tiles)
        return [pltpu.make_async_copy(
            gu_ref.at[lanes(place_of(q // tiles * 4 + r) * 512, 512, 512), :, lanes(core * inner + n * 512, 512, 512)],
            gub.at[s, pl.ds(r * 512, 512)], s_gu.at[s, r]) for r in range(4)]

    def column(t):
        k = t // 2
        y = jnp.where(k < 2, 1 - yz, yz)
        ch = jnp.where(k % 2 == 0, 1 - chip, chip)
        co = jnp.where(t % 2 == 0, 1 - core, core)
        return 2 * (2 * ch + co) + y

    def wd_copies(t):
        s = lax.rem(t, 3)
        rows = inner // 2
        return [pltpu.make_async_copy(wd_ref.at[lanes(core * inner + r * rows, rows, rows), lanes(column(t) * 512, 512, 512)],
                                      wd.at[s, pl.ds(r * rows, rows)], s_wd.at[s, r]) for r in range(2)]

    for copy in wo_copies:
        copy.start()
    greet((ynbr, xnbr, partner, far))

    slot = 2 * yz + core
    to_y = remote(o_ref.at[:, lanes((1 - yz) * half, half, 512)], og.at[slot], send.at[0], recv.at[0], ynbr)
    to_y.start()
    to_p = remote(o_ref.at[:, lanes(yz * half, half, 512)], og.at[slot], send.at[1], recv.at[1], partner)
    to_p.start()
    og[slot] = o_ref[:, lanes(yz * half, half, 512)]
    for q in range(3):
        for copy in gu_copies(jnp.int32(q)):
            copy.start()
    for t in range(3):
        for copy in wd_copies(jnp.int32(t)):
            copy.start()
    for copy in wo_copies:
        copy.wait()
    to_y.wait_recv()
    theirs = og.at[2 * (1 - yz) + core]
    onward = remote(theirs, theirs, send.at[2], recv.at[2], partner)
    onward.start()
    to_p.wait_recv()
    onward.wait_recv()

    def y_copy(e):
        return remote(ys.at[e], yr.at[e], ysend.at[e], yrecv.at[e], ynbr)

    @pl.loop(0, 2)
    def _(e):
        ys[e] = dot(og[...].reshape(256, half), wo[2 * (1 - yz) + e]).astype(jnp.bfloat16)
        y_copy(e).start()

    @pl.loop(0, 2)
    def _(e):
        own[e] = dot(og[...].reshape(256, half), wo[2 * yz + e])

    first = 4 * core + 2 * yz

    def h_send(e):
        return remote(h1.at[first + e], h1.at[first + e], hsend.at[e], hrecv.at[e], partner)

    def a_send(e):
        return remote(h1.at[first + e], h1.at[first + e], asend.at[e], arecv.at[e], ynbr)

    def onto(e):
        there = h1.at[4 * core + 2 * (1 - yz) + e]
        return remote(there, there, osend.at[e], orecv.at[e], partner)

    power = jnp.zeros((256, 1), jnp.float32)
    for e in range(2):
        y_copy(e).wait_recv()
        res = hres[:, :, e * 512:(e + 1) * 512].reshape(256, 512).astype(jnp.float32)
        hid = (res + (own[e] + yr[e].astype(jnp.float32))).astype(jnp.bfloat16)
        h1[first + e] = hid
        h_send(e).start()
        hid = hid.astype(jnp.float32)
        power += jnp.sum(hid * hid, axis=1, keepdims=True)

    at_lane = lax.broadcasted_iota(jnp.int32, (32, 8, 128), 2) == lax.broadcasted_iota(jnp.int32, (32, 8, 128), 0)
    st[slot] = jnp.sum(jnp.where(at_lane, power.reshape(32, 8, 1), 0.0), axis=0)
    stats = [remote(st.at[slot], st.at[slot], ssend.at[k], srecv.at[k], target)
             for k, target in enumerate((ynbr, far, partner))]
    for copy in stats:
        copy.start()
    for e in range(2):
        a_send(e).start()
    for copy in stats:
        copy.wait_recv()
    total = (st[0] + st[1]) + (st[2] + st[3])
    power = jnp.sum(jnp.where(at_lane, total[None], 0.0), axis=2, keepdims=True).reshape(256, 1)
    inv_ref[...] = jnp.broadcast_to(lax.rsqrt(power / model + NORM_EPS), (256, 128))

    at = lax.broadcasted_iota(jnp.int32, (128, 512), 1)
    spread = (at % 256 == 2 * lax.broadcasted_iota(jnp.int32, (128, 512), 0) + at // 256).astype(jnp.bfloat16)

    def prepare(p):
        b = place_of(p)
        gain = gain_ref[:, lanes(b * 512, 512, 512)].astype(jnp.float32)
        ubuf[...] = (h1[b].astype(jnp.float32) * inv_ref[:, :1] * gain).astype(jnp.bfloat16)
        for q in range(4):
            wide = dot(ubuf[:, q * 128:(q + 1) * 128], spread).astype(jnp.bfloat16)
            ue[:256, lanes(p * 1024 + q * 256, 256, 256)] = wide[:, :256]
            ue[256:, lanes(p * 1024 + q * 256, 256, 256)] = wide[:, 256:]

    for e in range(2):
        h_send(e).wait_recv()

    @pl.loop(0, 4)
    def _(p):
        prepare(p)

    def more(q):
        @pl.when(q + 3 < 2 * tiles)
        def _():
            for copy in gu_copies(q + 3):
                copy.start()

    @pl.loop(0, tiles)
    def _(n):
        @pl.when((n == 2) | (n == 4))
        def _():
            a_send(n // 2 - 1).wait_recv()
            onto(n // 2 - 1).start()

        for copy in gu_copies(n):
            copy.wait()
        gacc[n] = dot(ue[:, :model], gub.at[lax.rem(n, 3)].reshape(model, 512)[...])
        more(n)

    for e in range(2):
        onto(e).wait_recv()

    @pl.loop(4, 8)
    def _(p):
        prepare(p)

    @pl.loop(0, tiles)
    def _(n):
        q = n + tiles
        for copy in gu_copies(q):
            copy.wait()
        both = gacc[n] + dot(ue[:, model:], gub.at[lax.rem(q, 3)].reshape(model, 512)[...])
        more(q)
        gate = both[:256].astype(jnp.bfloat16).astype(jnp.float32)
        up = both[256:].astype(jnp.bfloat16).astype(jnp.float32)
        mbuf[:, lanes(n * 512, 512, 512)] = (gate * jax.nn.sigmoid(gate) * up).astype(jnp.bfloat16)

    def p_copy(k):
        return remote(ps.at[k], pr.at[k], psend.at[k], precv.at[k], partner)

    def f_copy(k):
        return remote(fs.at[k], fr.at[k], fsend.at[k], frecv.at[k], ynbr)

    x_copy = remote(xs, out_ref.at[:, chip], xsend.at[0], xrecv.at[0], xnbr)

    @pl.loop(0, 4)
    def _(k):
        for side in range(2):
            t = 2 * k + side
            s = lax.rem(t, 3)
            for copy in wd_copies(t):
                copy.wait()
            part = dot(mbuf[...], wd[s])

            @pl.when(t + 3 < 8)
            def _():
                for copy in wd_copies(t + 3):
                    copy.start()

            if side == 0:
                ps[k] = part.astype(jnp.bfloat16)
                p_copy(k).start()
            else:
                acc[...] = part
        p_copy(k).wait_recv()
        acc[...] += pr[k].astype(jnp.float32)

        @pl.when(k < 2)
        def _():
            fs[k] = acc[...].astype(jnp.bfloat16)
            f_copy(k).start()

        @pl.when(k >= 2)
        def _():
            f_copy(k - 2).wait_recv()
            total = acc[...] + fr[k - 2].astype(jnp.float32)
            final = (h1[column(2 * k + 1)].astype(jnp.float32) + total).astype(jnp.bfloat16).reshape(2, 128, 512)

            @pl.when(k == 2)
            def _():
                xs[...] = final
                x_copy.start()

            @pl.when(k == 3)
            def _():
                out_ref[:, chip] = final

    x_copy.wait()
    for copy in (to_y, to_p, onward):
        copy.wait_send()

    for copy in stats:
        copy.wait_send()
    for n in range(4):
        p_copy(n).wait_send()
    for n in range(2):
        for copy in (y_copy(n), h_send(n), a_send(n), onto(n), f_copy(n)):
            copy.wait_send()


def mlp(o, hres, gain, w_out, w_gate_up, w_down):
    half, model = w_out.shape
    inner = w_gate_up.shape[2] // 2
    anywhere = pl.BlockSpec(memory_space=pl.ANY)
    vmem = pl.BlockSpec(memory_space=VMEM)
    bf16 = jnp.bfloat16
    out = pl.pallas_call(
        mlp_kernel,
        out_shape=jax.ShapeDtypeStruct((2, 2, 128, 512), bf16),
        in_specs=[vmem, vmem, vmem, anywhere, anywhere, anywhere],
        out_specs=vmem,
        scratch_shapes=[
            VMEM((4, 64, half), bf16), VMEM((4, half, 512), bf16),
            VMEM((2, 256, 512), bf16), VMEM((2, 256, 512), bf16), VMEM((2, 256, 512), jnp.float32), VMEM((8, 256, 512), bf16),
            VMEM((256, 128), jnp.float32), VMEM((256, 512), bf16), VMEM((512, 2 * model), bf16),
            VMEM((3, half, 2, 512), bf16), VMEM((inner // 512, 512, 512), jnp.float32),
            VMEM((256, inner), bf16), VMEM((3, inner, 512), bf16),
            VMEM((4, 256, 512), bf16), VMEM((4, 256, 512), bf16), VMEM((256, 512), jnp.float32),
            VMEM((2, 256, 512), bf16), VMEM((2, 256, 512), bf16), VMEM((2, 128, 512), bf16), VMEM((4, 8, 128), jnp.float32),
            DMA((4,)), DMA((3, 4)), DMA((3, 2)),
            DMA((3,)), DMA((3,)), DMA((2,)), DMA((2,)), DMA((2,)), DMA((2,)), DMA((2,)), DMA((2,)), DMA((2,)), DMA((2,)),
            DMA((3,)), DMA((3,)),
            DMA((4,)), DMA((4,)), DMA((2,)), DMA((2,)), DMA((1,)), DMA((1,)),
        ],
        compiler_params=pltpu.CompilerParams(collective_id=1, has_side_effects=True, vmem_limit_bytes=60 * MIB),
        name='mlp',
    )(o, hres, gain, w_out, w_gate_up, w_down)
    return out.reshape(512, 512)


def move_kernel(h_ref, out_ref, sem):
    copy = pltpu.make_async_copy(h_ref, out_ref, sem)
    copy.start()
    copy.wait()


def move(hidden):
    return pl.pallas_call(
        move_kernel,
        out_shape=jax.ShapeDtypeStruct(hidden.shape, hidden.dtype),
        in_specs=[pl.BlockSpec(memory_space=VMEM)],
        out_specs=pl.BlockSpec(memory_space=pl.ANY),
        scratch_shapes=[DMA],
        name='move',
    )(hidden)


def solution(mesh):
    batch_axes = ('replica', 'yz', 'x')
    hidden_spec = P('replica', ('x', 'yz'))
    cache_spec = P(None, batch_axes, None, None)

    def local_step(hidden, seq_lens, attn_gain, mlp_gain, w_qkv, w_out, w_gate_up, w_down, k_cache, v_cache):
        k_layers = []
        v_layers = []
        for layer in range(w_qkv.shape[0]):
            z, hres = project_qkv(hidden, attn_gain[layer:layer + 1], w_qkv[layer])
            o, k_upd, v_upd = attend(seq_lens, by_length(seq_lens), z, k_cache[layer], v_cache[layer])
            k_layers.append(k_upd)
            v_layers.append(v_upd)
            hidden = mlp(o, hres, mlp_gain[layer:layer + 1], w_out[layer], w_gate_up[layer], w_down[layer])
        return move(hidden), jnp.stack(k_layers), jnp.stack(v_layers)

    return jax.shard_map(
        local_step,
        mesh=mesh,
        in_specs=(hidden_spec, P(batch_axes), P(None, None), P(None, None), P(None, None, 'yz'), P(None, 'yz', None),
                  P(None, None, None, 'yz'), P(None, 'yz', None), cache_spec, cache_spec),
        out_specs=(hidden_spec, cache_spec, cache_spec),
        check_vma=False)
```

```python
import functools

import jax
import jax.numpy as jnp
from jax import lax
from jax.experimental import pallas as pl
from jax.experimental.pallas import tpu as pltpu
from jax.sharding import PartitionSpec as P

NORM_EPS = 1e-5
MESH = pl.DeviceIdType.MESH
MIB = 1 << 20
GROUP, DEPTH = 4, 4
EARLY = 16
VMEM = pltpu.VMEM
DMA = pltpu.SemaphoreType.DMA


def place():
    yz = lax.axis_index('yz')
    x = lax.axis_index('x')
    return yz, x // 2, x % 2


def device(yz, chip, core):
    return {'yz': yz, 'x': 2 * chip + core}


def remote(src, dst, send, recv, target):
    return pltpu.make_async_remote_copy(src_ref=src, dst_ref=dst, send_sem=send, recv_sem=recv,
                                        device_id=target, device_id_type=MESH)


def greet(peers):
    barrier = pltpu.get_barrier_semaphore()
    for peer in peers:
        pl.semaphore_signal(barrier, inc=1, device_id=peer, device_id_type=MESH)
    pl.semaphore_wait(barrier, len(peers))


def lanes(start, size, unit=128):
    return pl.ds(pl.multiple_of(start, unit), size)


def slot_columns(yz, core):
    return core * 2048 + yz * 1024


def dot(a, b):
    return jnp.dot(a, b, preferred_element_type=jnp.float32)


def early_kernel(order_ref, k_ref, v_ref, ko_ref, vo_ref, kbuf, vbuf, isem, osem, *, count, slots, ahead):
    def moves(t, into):
        s = lax.rem(t, slots)
        b = order_ref[(t // GROUP * 4 + 2) * GROUP + lax.rem(t, GROUP)]
        if into:
            return (pltpu.make_async_copy(k_ref.at[b], kbuf.at[s], isem.at[0, s]),
                    pltpu.make_async_copy(v_ref.at[b], vbuf.at[s], isem.at[1, s]))
        return (pltpu.make_async_copy(kbuf.at[s], ko_ref.at[b], osem.at[0, s]),
                pltpu.make_async_copy(vbuf.at[s], vo_ref.at[b], osem.at[1, s]))

    @pl.loop(0, ahead)
    def _(t):
        for copy in moves(t, True):
            copy.start()

    @pl.loop(0, count)
    def _(t):
        @pl.when(t + ahead < count)
        def _():
            @pl.when(t + ahead >= slots)
            def _():
                for copy in moves(t + ahead - slots, False):
                    copy.wait()
            for copy in moves(t + ahead, True):
                copy.start()

        for copy in moves(t, True):
            copy.wait()
        for copy in moves(t, False):
            copy.start()

    @pl.loop(max(count - slots, 0), count)
    def _(t):
        for copy in moves(t, False):
            copy.wait()


def copy_early(order, k_cache, v_cache):
    anywhere = pl.BlockSpec(memory_space=pl.ANY)
    slots, ahead = 16, 8
    return pl.pallas_call(
        functools.partial(early_kernel, count=EARLY, slots=slots, ahead=ahead),
        out_shape=tuple(jax.ShapeDtypeStruct(x.shape, x.dtype) for x in (k_cache, v_cache)),
        in_specs=[pl.BlockSpec(memory_space=pltpu.SMEM), anywhere, anywhere],
        out_specs=(anywhere, anywhere),
        scratch_shapes=[VMEM((slots,) + k_cache.shape[1:], jnp.bfloat16), VMEM((slots,) + k_cache.shape[1:], jnp.bfloat16),
                        DMA((2, slots)), DMA((2, slots))],
        cost_estimate=pl.CostEstimate(flops=10 ** 11, bytes_accessed=4 * EARLY * k_cache[0].size * 2, transcendentals=0),
        compiler_params=pltpu.CompilerParams(vmem_limit_bytes=40 * MIB),
        name='copy_early',
    )(order, k_cache, v_cache)


def qkv_kernel(own_ref, by_ref, bx_ref, bd_ref, gain_ref, w_ref, _, z_ref, hres_ref, hx_ref, wbuf, ubuf, zbuf,
               w_sem, send, recv, zsend, zrecv):
    yz, chip, core = place()
    cols = own_ref.shape[-1]
    width = z_ref.shape[-1]
    parts = ((0, 512), (512, width - 512))
    step = w_ref.shape[1] - width
    model = hx_ref.shape[-1]
    loads = []
    for n, (off, size) in enumerate(parts):
        loads.append(pltpu.make_async_copy(w_ref.at[:, lanes(core * step + off, size)],
                                           wbuf.at[:, pl.ds(off, size)], w_sem.at[n]))
        loads[-1].start()
    ynbr, partner = device(1 - yz, chip, core), device(yz, chip, 1 - core)
    far = device(1 - yz, chip, 1 - core)
    greet((ynbr, partner, far))
    copies = []
    blocks = ((own_ref, yz, chip), (by_ref, 1 - yz, chip), (bx_ref, yz, 1 - chip), (bd_ref, 1 - yz, 1 - chip))
    for k, (ref, y, ch) in enumerate(blocks):
        here = lanes((2 * (2 * ch + core) + y) * cols, cols, 512)
        copies.append(remote(ref, hx_ref.at[:, :, here], send.at[k], recv.at[k], partner))
        copies[-1].start()
    for ref, y, ch in blocks:
        hx_ref[:, :, lanes((2 * (2 * ch + core) + y) * cols, cols, 512)] = ref[...]
    for copy in copies:
        copy.wait_recv()

    gain = gain_ref[...].astype(jnp.float32)
    chunk = 32
    for half in range(2):
        @pl.loop(0, 128 // chunk)
        def _(r):
            hid = hx_ref[half, lanes(r * chunk, chunk, chunk), :].astype(jnp.float32)
            inv = lax.rsqrt(jnp.sum(hid * hid, axis=1, keepdims=True) / model + NORM_EPS)
            ubuf[lanes(half * 128 + r * chunk, chunk, chunk), :] = (hid * inv * gain).astype(jnp.bfloat16)

    slot = 2 * yz + core
    zcopies = []
    for n, (off, size) in enumerate(parts):
        loads[n].wait()
        z = dot(ubuf[...], wbuf[:, off:off + size]).astype(jnp.bfloat16)
        zbuf[:, :, off:off + size] = z.reshape(4, 64, size)
        for k, (y, co, target) in enumerate(((1 - yz, core, ynbr), (1 - yz, 1 - core, far), (yz, 1 - core, partner))):
            zcopies.append(remote(zbuf.at[2 * y + co, :, pl.ds(off, size)], z_ref.at[slot, :, pl.ds(off, size)],
                                  zsend.at[n, k], zrecv.at[n, k], target))
            zcopies[-1].start()
    z_ref[slot] = zbuf[slot]
    hres_ref[...] = hx_ref[:, :, lanes(slot_columns(yz, core), 1024, 512)]
    for copy in copies:
        copy.wait_send()
    for copy in zcopies:
        copy.wait()


def project_qkv(blocks, gain, w_qkv, after):
    model, half = w_qkv.shape
    width = (half // 128 + 1) // 2 * 128
    vmem = pl.BlockSpec(memory_space=VMEM)
    anywhere = pl.BlockSpec(memory_space=pl.ANY)
    return pl.pallas_call(
        qkv_kernel,
        out_shape=(jax.ShapeDtypeStruct((4, 64, width), jnp.bfloat16),
                   jax.ShapeDtypeStruct((2, 128, model // 4), jnp.bfloat16)),
        in_specs=[vmem, vmem, vmem, vmem, vmem, anywhere, anywhere],
        out_specs=(pl.BlockSpec(memory_space=VMEM), pl.BlockSpec(memory_space=VMEM)),
        scratch_shapes=[VMEM((2, 128, model), jnp.bfloat16), VMEM((model, width), jnp.bfloat16), VMEM((256, model), jnp.bfloat16),
                        VMEM((4, 64, width), jnp.bfloat16), DMA((2,)), DMA((4,)), DMA((4,)), DMA((2, 3)), DMA((2, 3))],
        compiler_params=pltpu.CompilerParams(collective_id=0, has_side_effects=True, vmem_limit_bytes=40 * MIB),
        name='qkv',
    )(*blocks, gain, w_qkv, after)


def attention_kernel(lens_ref, order_ref, z_ref, k_ref, v_ref, _, __, o_ref, ko_ref, vo_ref,
                     qs, kn, vn, os, kbuf, vbuf, sem, fsem, *, heads, group, depth, unit):
    seqs, length, dim = k_ref.shape
    tiles = (heads + 2) // 2
    split = tiles // 2
    groups = seqs // group
    sizes = length // unit

    def tile(t):
        y, local = t // tiles, t % tiles
        co = 1 if local >= split else 0
        first = (local - split * co) * dim
        return z_ref[2 * y + co, :, first:first + dim].astype(jnp.float32)

    def by_size(g, act):
        need = lens_ref[order_ref[g * group]] // unit + 1
        for size in range(1, sizes + 1):
            @pl.when(need == size)
            def _():
                act(size * unit)

    def fetch(g, rows):
        out = []
        for m in range(group):
            b = order_ref[g * group + m]
            s = lax.rem(g, depth) * group + m
            out.append(pltpu.make_async_copy(k_ref.at[b, pl.ds(0, rows)], kbuf.at[s, pl.ds(0, rows)], sem.at[0, s]))
            out.append(pltpu.make_async_copy(v_ref.at[b, pl.ds(0, rows)], vbuf.at[s, pl.ds(0, rows)], sem.at[1, s]))
        return out

    def flush(g, act):
        def tail(rows_of):
            for m in range(group):
                b = order_ref[g * group + m]
                s = lax.rem(g, depth) * group + m
                rows = rows_of(b)
                act(pltpu.make_async_copy(kbuf.at[s, rows], ko_ref.at[b, rows], fsem.at[0, s]))
                act(pltpu.make_async_copy(vbuf.at[s, rows], vo_ref.at[b, rows], fsem.at[1, s]))

        @pl.when(lax.rem(g, 4) != 2)
        def _():
            tail(lambda b: pl.ds(0, length))

        @pl.when(lax.rem(g, 4) == 2)
        def _():
            tail(lambda b: lanes(lens_ref[b] // 16 * 16, 16, 16))

    def arrive(g, begin):
        def act(rows):
            for copy in fetch(g, rows):
                if begin:
                    copy.start()
                else:
                    copy.wait()

        @pl.when(lax.rem(g, 4) != 2)
        def _():
            act(length)

        @pl.when(lax.rem(g, 4) == 2)
        def _():
            by_size(g, act)

    for g in range(2):
        arrive(jnp.int32(g), True)
    for t in range(heads):
        qs[pl.ds(t, seqs, stride=heads), :] = tile(t)
    kn[...] = tile(heads)
    vn[...] = tile(heads + 1)

    @pl.loop(0, groups)
    def _(g):
        @pl.when(g >= depth - 2)
        def _():
            flush(g - (depth - 2), lambda copy: copy.wait())

        @pl.when(g + 2 < groups)
        def _():
            arrive(g + 2, True)

        arrive(g, False)
        for m in range(group):
            b = order_ref[g * group + m]
            s = lax.rem(g, depth) * group + m
            last = lens_ref[b]
            base = pl.multiple_of(last // 16 * 16, 16)
            row = lax.broadcasted_iota(jnp.int32, (16, dim), 0) == last - base
            for buf, new in ((kbuf, kn), (vbuf, vn)):
                old = buf[s, pl.ds(base, 16), :].astype(jnp.float32)
                buf[s, pl.ds(base, 16), :] = jnp.where(row, new[pl.ds(b, 1), :], old).astype(jnp.bfloat16)

        flush(g, lambda copy: copy.start())

        def act(rows):
            scores = []
            for m in range(group):
                b = order_ref[g * group + m]
                s = lax.rem(g, depth) * group + m
                q = qs[lanes(b * heads, heads, heads), :].astype(jnp.bfloat16)
                raw = lax.dot_general(q, kbuf[s, :rows], (((1,), (1,)), ((), ())), preferred_element_type=jnp.float32)
                seen = lax.broadcasted_iota(jnp.int32, (heads, rows), 1) <= lens_ref[b]
                scores.append(jnp.where(seen, raw * dim ** -0.5, -1e30))
            tops = [jnp.max(x, axis=1, keepdims=True) for x in scores]
            probs = [jnp.exp(x - top) for x, top in zip(scores, tops)]
            sums = [1.0 / jnp.sum(x, axis=1, keepdims=True) for x in probs]
            for m in range(group):
                b = order_ref[g * group + m]
                s = lax.rem(g, depth) * group + m
                os[lanes(b * heads, heads, heads), :] = dot((probs[m] * sums[m]).astype(jnp.bfloat16), vbuf[s, :rows])

        by_size(g, act)

    for t in range(heads):
        o_ref[:, t * dim:(t + 1) * dim] = os[pl.ds(t, seqs, stride=heads), :].astype(jnp.bfloat16)

    @pl.loop(groups - (depth - 2), groups)
    def _(g):
        flush(g, lambda copy: copy.wait())


def by_length(lens):
    seqs = lens.shape[0]
    ids = jnp.arange(seqs)
    ahead = (lens[None, :] > lens[:, None]) | ((lens[None, :] == lens[:, None]) & (ids[None, :] < ids[:, None]))
    rank = jnp.sum(ahead.astype(jnp.int32), axis=1)
    late = (seqs - EARLY) // GROUP
    place_in = rank // GROUP
    place_in = jnp.where(place_in < late, place_in + (place_in + 1) // 3, 4 * (place_in - late) + 2)
    place_in = place_in * GROUP + rank % GROUP
    return jnp.sum(jnp.where(place_in[None, :] == ids[:, None], ids[None, :], 0), axis=1).astype(jnp.int32)


def attend(lens, order, z, k_cache, v_cache, k_out, v_out):
    seqs, length, dim = k_cache.shape
    heads = 32
    group, depth, unit = GROUP, DEPTH, 256
    anywhere = pl.BlockSpec(memory_space=pl.ANY)
    vmem = pl.BlockSpec(memory_space=VMEM)
    smem = pl.BlockSpec(memory_space=pltpu.SMEM)
    return pl.pallas_call(
        functools.partial(attention_kernel, heads=heads, group=group, depth=depth, unit=unit),
        out_shape=(jax.ShapeDtypeStruct((seqs, heads * dim), jnp.bfloat16),
                   jax.ShapeDtypeStruct(k_cache.shape, k_cache.dtype), jax.ShapeDtypeStruct(v_cache.shape, v_cache.dtype)),
        in_specs=[smem, smem, vmem, anywhere, anywhere, anywhere, anywhere],
        out_specs=(vmem, anywhere, anywhere),
        input_output_aliases={5: 1, 6: 2},
        scratch_shapes=[VMEM((seqs * heads, dim), jnp.float32), VMEM((seqs, dim), jnp.float32),
                        VMEM((seqs, dim), jnp.float32), VMEM((seqs * heads, dim), jnp.float32),
                        VMEM((group * depth, length, dim), jnp.bfloat16), VMEM((group * depth, length, dim), jnp.bfloat16),
                        DMA((2, group * depth)), DMA((2, group * depth))],
        compiler_params=pltpu.CompilerParams(vmem_limit_bytes=50 * MIB),
        name='attention',
    )(lens, order, z, k_cache, v_cache, k_out, v_out)


def mlp_kernel(o_ref, hres, gain_ref, wo_ref, gu_ref, wd_ref, out_ref,
               og, wo, ys, yr, own, h1, inv_ref, ubuf, ue, gub, gacc, mbuf, wd, ps, pr, acc, fs, fr, xs, st,
               s_wo, s_gu, s_wd, send, recv, ysend, yrecv, hsend, hrecv, asend, arecv, osend, orecv, ssend, srecv,
               psend, precv, fsend, frecv, xsend, xrecv):
    yz, chip, core = place()
    half = wo_ref.shape[0]
    model = wo_ref.shape[1]
    inner = gu_ref.shape[2] // 2
    tiles = inner // 512
    ynbr, xnbr, partner = device(1 - yz, chip, core), device(yz, 1 - chip, core), device(yz, chip, 1 - core)
    far = device(1 - yz, chip, 1 - core)

    wo_copies = [pltpu.make_async_copy(wo_ref.at[:, lanes(core * half + n * 512, 512, 512)], wo.at[n], s_wo.at[n])
                 for n in range(4)]

    def place_of(p):
        y = jnp.where(p < 4, yz, 1 - yz)
        return (p % 4) // 2 * 4 + 2 * y + p % 2

    def gu_copies(q):
        s = lax.rem(q, 3)
        n = lax.rem(q, tiles)
        return [pltpu.make_async_copy(
            gu_ref.at[lanes(place_of(q // tiles * 4 + r) * 512, 512, 512), :, lanes(core * inner + n * 512, 512, 512)],
            gub.at[s, pl.ds(r * 512, 512)], s_gu.at[s, r]) for r in range(4)]

    def column(t):
        k = t // 2
        y = jnp.where(k < 2, 1 - yz, yz)
        ch = jnp.where(k % 2 == 0, 1 - chip, chip)
        co = jnp.where(t % 2 == 0, 1 - core, core)
        return 2 * (2 * ch + co) + y

    def wd_copies(t):
        s = lax.rem(t, 3)
        rows = inner // 2
        return [pltpu.make_async_copy(wd_ref.at[lanes(core * inner + r * rows, rows, rows), lanes(column(t) * 512, 512, 512)],
                                      wd.at[s, pl.ds(r * rows, rows)], s_wd.at[s, r]) for r in range(2)]

    for copy in wo_copies:
        copy.start()
    greet((ynbr, xnbr, partner, far))

    slot = 2 * yz + core
    to_y = remote(o_ref.at[:, lanes((1 - yz) * half, half, 512)], og.at[slot], send.at[0], recv.at[0], ynbr)
    to_y.start()
    to_p = remote(o_ref.at[:, lanes(yz * half, half, 512)], og.at[slot], send.at[1], recv.at[1], partner)
    to_p.start()
    og[slot] = o_ref[:, lanes(yz * half, half, 512)]
    for q in range(3):
        for copy in gu_copies(jnp.int32(q)):
            copy.start()
    for t in range(3):
        for copy in wd_copies(jnp.int32(t)):
            copy.start()
    for copy in wo_copies:
        copy.wait()
    to_y.wait_recv()
    theirs = og.at[2 * (1 - yz) + core]
    onward = remote(theirs, theirs, send.at[2], recv.at[2], partner)
    onward.start()
    to_p.wait_recv()
    onward.wait_recv()

    def y_copy(e):
        return remote(ys.at[e], yr.at[e], ysend.at[e], yrecv.at[e], ynbr)

    @pl.loop(0, 2)
    def _(e):
        ys[e] = dot(og[...].reshape(256, half), wo[2 * (1 - yz) + e]).astype(jnp.bfloat16)
        y_copy(e).start()

    @pl.loop(0, 2)
    def _(e):
        own[e] = dot(og[...].reshape(256, half), wo[2 * yz + e])

    first = 4 * core + 2 * yz

    def h_send(e):
        return remote(h1.at[first + e], h1.at[first + e], hsend.at[e], hrecv.at[e], partner)

    def a_send(e):
        return remote(h1.at[first + e], h1.at[first + e], asend.at[e], arecv.at[e], ynbr)

    def onto(e):
        there = h1.at[4 * core + 2 * (1 - yz) + e]
        return remote(there, there, osend.at[e], orecv.at[e], partner)

    power = jnp.zeros((256, 1), jnp.float32)
    for e in range(2):
        y_copy(e).wait_recv()
        res = hres[:, :, e * 512:(e + 1) * 512].reshape(256, 512).astype(jnp.float32)
        hid = (res + (own[e] + yr[e].astype(jnp.float32))).astype(jnp.bfloat16)
        h1[first + e] = hid
        h_send(e).start()
        hid = hid.astype(jnp.float32)
        power += jnp.sum(hid * hid, axis=1, keepdims=True)

    at_lane = lax.broadcasted_iota(jnp.int32, (32, 8, 128), 2) == lax.broadcasted_iota(jnp.int32, (32, 8, 128), 0)
    st[slot] = jnp.sum(jnp.where(at_lane, power.reshape(32, 8, 1), 0.0), axis=0)
    stats = [remote(st.at[slot], st.at[slot], ssend.at[k], srecv.at[k], target)
             for k, target in enumerate((ynbr, far, partner))]
    for copy in stats:
        copy.start()
    for e in range(2):
        a_send(e).start()
    for copy in stats:
        copy.wait_recv()
    total = (st[0] + st[1]) + (st[2] + st[3])
    power = jnp.sum(jnp.where(at_lane, total[None], 0.0), axis=2, keepdims=True).reshape(256, 1)
    inv_ref[...] = jnp.broadcast_to(lax.rsqrt(power / model + NORM_EPS), (256, 128))

    at = lax.broadcasted_iota(jnp.int32, (128, 512), 1)
    spread = (at % 256 == 2 * lax.broadcasted_iota(jnp.int32, (128, 512), 0) + at // 256).astype(jnp.bfloat16)

    def prepare(p):
        b = place_of(p)
        gain = gain_ref[:, lanes(b * 512, 512, 512)].astype(jnp.float32)
        ubuf[...] = (h1[b].astype(jnp.float32) * inv_ref[:, :1] * gain).astype(jnp.bfloat16)
        for q in range(4):
            wide = dot(ubuf[:, q * 128:(q + 1) * 128], spread).astype(jnp.bfloat16)
            ue[:256, lanes(p * 1024 + q * 256, 256, 256)] = wide[:, :256]
            ue[256:, lanes(p * 1024 + q * 256, 256, 256)] = wide[:, 256:]

    for e in range(2):
        h_send(e).wait_recv()

    @pl.loop(0, 4)
    def _(p):
        prepare(p)

    def more(q):
        @pl.when(q + 3 < 2 * tiles)
        def _():
            for copy in gu_copies(q + 3):
                copy.start()

    @pl.loop(0, tiles)
    def _(n):
        @pl.when((n == 2) | (n == 4))
        def _():
            a_send(n // 2 - 1).wait_recv()
            onto(n // 2 - 1).start()

        for copy in gu_copies(n):
            copy.wait()
        gacc[n] = dot(ue[:, :model], gub.at[lax.rem(n, 3)].reshape(model, 512)[...])
        more(n)

    for e in range(2):
        onto(e).wait_recv()

    @pl.loop(4, 8)
    def _(p):
        prepare(p)

    @pl.loop(0, tiles)
    def _(n):
        q = n + tiles
        for copy in gu_copies(q):
            copy.wait()
        both = gacc[n] + dot(ue[:, model:], gub.at[lax.rem(q, 3)].reshape(model, 512)[...])
        more(q)
        gate = both[:256].astype(jnp.bfloat16).astype(jnp.float32)
        up = both[256:].astype(jnp.bfloat16).astype(jnp.float32)
        mbuf[:, lanes(n * 512, 512, 512)] = (gate * jax.nn.sigmoid(gate) * up).astype(jnp.bfloat16)

    def p_copy(k):
        return remote(ps.at[k], pr.at[k], psend.at[k], precv.at[k], partner)

    def f_copy(k):
        return remote(fs.at[k], fr.at[k], fsend.at[k], frecv.at[k], ynbr)

    x_copy = remote(xs, out_ref.at[:, chip], xsend.at[0], xrecv.at[0], xnbr)

    @pl.loop(0, 4)
    def _(k):
        for side in range(2):
            t = 2 * k + side
            s = lax.rem(t, 3)
            for copy in wd_copies(t):
                copy.wait()
            part = dot(mbuf[...], wd[s])

            @pl.when(t + 3 < 8)
            def _():
                for copy in wd_copies(t + 3):
                    copy.start()

            if side == 0:
                ps[k] = part.astype(jnp.bfloat16)
                p_copy(k).start()
            else:
                acc[...] = part
        p_copy(k).wait_recv()
        acc[...] += pr[k].astype(jnp.float32)

        @pl.when(k < 2)
        def _():
            fs[k] = acc[...].astype(jnp.bfloat16)
            f_copy(k).start()

        @pl.when(k >= 2)
        def _():
            f_copy(k - 2).wait_recv()
            total = acc[...] + fr[k - 2].astype(jnp.float32)
            final = (h1[column(2 * k + 1)].astype(jnp.float32) + total).astype(jnp.bfloat16).reshape(2, 128, 512)

            @pl.when(k == 2)
            def _():
                xs[...] = final
                x_copy.start()

            @pl.when(k == 3)
            def _():
                out_ref[:, chip] = final

    x_copy.wait()
    for copy in (to_y, to_p, onward):
        copy.wait_send()

    for copy in stats:
        copy.wait_send()
    for n in range(4):
        p_copy(n).wait_send()
    for n in range(2):
        for copy in (y_copy(n), h_send(n), a_send(n), onto(n), f_copy(n)):
            copy.wait_send()


def mlp(o, hres, gain, w_out, w_gate_up, w_down):
    half, model = w_out.shape
    inner = w_gate_up.shape[2] // 2
    anywhere = pl.BlockSpec(memory_space=pl.ANY)
    vmem = pl.BlockSpec(memory_space=VMEM)
    bf16 = jnp.bfloat16
    out = pl.pallas_call(
        mlp_kernel,
        out_shape=jax.ShapeDtypeStruct((2, 2, 128, 512), bf16),
        in_specs=[vmem, vmem, vmem, anywhere, anywhere, anywhere],
        out_specs=vmem,
        scratch_shapes=[
            VMEM((4, 64, half), bf16), VMEM((4, half, 512), bf16),
            VMEM((2, 256, 512), bf16), VMEM((2, 256, 512), bf16), VMEM((2, 256, 512), jnp.float32), VMEM((8, 256, 512), bf16),
            VMEM((256, 128), jnp.float32), VMEM((256, 512), bf16), VMEM((512, 2 * model), bf16),
            VMEM((3, half, 2, 512), bf16), VMEM((inner // 512, 512, 512), jnp.float32),
            VMEM((256, inner), bf16), VMEM((3, inner, 512), bf16),
            VMEM((4, 256, 512), bf16), VMEM((4, 256, 512), bf16), VMEM((256, 512), jnp.float32),
            VMEM((2, 256, 512), bf16), VMEM((2, 256, 512), bf16), VMEM((2, 128, 512), bf16), VMEM((4, 8, 128), jnp.float32),
            DMA((4,)), DMA((3, 4)), DMA((3, 2)),
            DMA((3,)), DMA((3,)), DMA((2,)), DMA((2,)), DMA((2,)), DMA((2,)), DMA((2,)), DMA((2,)), DMA((2,)), DMA((2,)),
            DMA((3,)), DMA((3,)),
            DMA((4,)), DMA((4,)), DMA((2,)), DMA((2,)), DMA((1,)), DMA((1,)),
        ],
        compiler_params=pltpu.CompilerParams(collective_id=1, has_side_effects=True, vmem_limit_bytes=60 * MIB),
        name='mlp',
    )(o, hres, gain, w_out, w_gate_up, w_down)
    return out.reshape(512, 512)


def move_kernel(h_ref, out_ref, sem):
    copy = pltpu.make_async_copy(h_ref, out_ref, sem)
    copy.start()
    copy.wait()


def move(hidden):
    return pl.pallas_call(
        move_kernel,
        out_shape=jax.ShapeDtypeStruct(hidden.shape, hidden.dtype),
        in_specs=[pl.BlockSpec(memory_space=VMEM)],
        out_specs=pl.BlockSpec(memory_space=pl.ANY),
        scratch_shapes=[DMA],
        name='move',
    )(hidden)


def solution(mesh):
    batch_axes = ('replica', 'yz', 'x')
    hidden_spec = P('replica', ('x', 'yz'))
    cache_spec = P(None, batch_axes, None, None)

    def local_step(hidden, seq_lens, attn_gain, mlp_gain, w_qkv, w_out, w_gate_up, w_down, k_cache, v_cache):
        k_layers = []
        v_layers = []
        for layer in range(w_qkv.shape[0]):
            order = by_length(seq_lens)
            rows = hidden.reshape(2, 2, 128, hidden.shape[1])
            chip = lax.axis_index('x') // 2
            own = lax.dynamic_index_in_dim(rows, chip, 1, keepdims=False)
            other = lax.dynamic_index_in_dim(rows, 1 - chip, 1, keepdims=False)
            by = lax.ppermute(own, 'yz', [(0, 1), (1, 0)])
            bx = lax.ppermute(other, 'x', [(j, j ^ 2) for j in range(4)])
            bd = lax.ppermute(other, ('yz', 'x'), [(j, j ^ 6) for j in range(8)])
            k_upd, v_upd = copy_early(order, k_cache[layer], v_cache[layer])
            z, hres = project_qkv((own, by, bx, bd), attn_gain[layer:layer + 1], w_qkv[layer], k_upd)
            o, k_upd, v_upd = attend(seq_lens, order, z, k_cache[layer], v_cache[layer], k_upd, v_upd)
            k_layers.append(k_upd)
            v_layers.append(v_upd)
            hidden = mlp(o, hres, mlp_gain[layer:layer + 1], w_out[layer], w_gate_up[layer], w_down[layer])
        return move(hidden), jnp.stack(k_layers), jnp.stack(v_layers)

    return jax.shard_map(
        local_step,
        mesh=mesh,
        in_specs=(hidden_spec, P(batch_axes), P(None, None), P(None, None), P(None, None, 'yz'), P(None, 'yz', None),
                  P(None, None, None, 'yz'), P(None, 'yz', None), cache_spec, cache_spec),
        out_specs=(hidden_spec, cache_spec, cache_spec),
        check_vma=False)
```

```python
import functools

import jax
import jax.numpy as jnp
from jax import lax
from jax.experimental import pallas as pl
from jax.experimental.pallas import tpu as pltpu
from jax.sharding import PartitionSpec as P

NORM_EPS = 1e-5
MESH = pl.DeviceIdType.MESH
MIB = 1 << 20
GROUP, DEPTH = 4, 4
EARLY = 16
COLS, ROWS, LANE, PAIR, SEQS = 512, 256, 128, 1024, 64
VMEM = pltpu.VMEM
DMA = pltpu.SemaphoreType.DMA
ONE = DMA((1,))
TWO = DMA((2,))
THREE = DMA((3,))
FOUR = DMA((4,))


def place():
    yz = lax.axis_index('yz')
    x = lax.axis_index('x')
    return yz, x // 2, x % 2


def device(yz, chip, core):
    return {'yz': yz, 'x': 2 * chip + core}


def remote(src, dst, send, recv, target):
    return pltpu.make_async_remote_copy(src_ref=src, dst_ref=dst, send_sem=send, recv_sem=recv,
                                        device_id=target, device_id_type=MESH)


def greet(peers):
    barrier = pltpu.get_barrier_semaphore()
    for peer in peers:
        pl.semaphore_signal(barrier, inc=1, device_id=peer, device_id_type=MESH)
    pl.semaphore_wait(barrier, len(peers))


def lanes(start, size, unit=128):
    return pl.ds(pl.multiple_of(start, unit), size)


def slot_columns(yz, core):
    return core * 2048 + yz * 1024


def dot(a, b):
    return jnp.dot(a, b, preferred_element_type=jnp.float32)


def early_kernel(order_ref, k_ref, v_ref, ko_ref, vo_ref, kbuf, vbuf, isem, osem, *, count, slots, ahead):
    def moves(t, into):
        s = lax.rem(t, slots)
        b = order_ref[(t // GROUP * 4 + 2) * GROUP + lax.rem(t, GROUP)]
        if into:
            return (pltpu.make_async_copy(k_ref.at[b], kbuf.at[s], isem.at[0, s]),
                    pltpu.make_async_copy(v_ref.at[b], vbuf.at[s], isem.at[1, s]))
        return (pltpu.make_async_copy(kbuf.at[s], ko_ref.at[b], osem.at[0, s]),
                pltpu.make_async_copy(vbuf.at[s], vo_ref.at[b], osem.at[1, s]))

    @pl.loop(0, ahead)
    def _(t):
        for copy in moves(t, True):
            copy.start()

    @pl.loop(0, count)
    def _(t):
        @pl.when(t + ahead < count)
        def _():
            @pl.when(t + ahead >= slots)
            def _():
                for copy in moves(t + ahead - slots, False):
                    copy.wait()
            for copy in moves(t + ahead, True):
                copy.start()

        for copy in moves(t, True):
            copy.wait()
        for copy in moves(t, False):
            copy.start()

    @pl.loop(max(count - slots, 0), count)
    def _(t):
        for copy in moves(t, False):
            copy.wait()


def copy_early(order, k_cache, v_cache):
    anywhere = pl.BlockSpec(memory_space=pl.ANY)
    slots, ahead = 16, 8
    return pl.pallas_call(
        functools.partial(early_kernel, count=EARLY, slots=slots, ahead=ahead),
        out_shape=tuple(jax.ShapeDtypeStruct(x.shape, x.dtype) for x in (k_cache, v_cache)),
        in_specs=[pl.BlockSpec(memory_space=pltpu.SMEM), anywhere, anywhere],
        out_specs=(anywhere, anywhere),
        scratch_shapes=[VMEM((slots,) + k_cache.shape[1:], jnp.bfloat16), VMEM((slots,) + k_cache.shape[1:], jnp.bfloat16),
                        DMA((2, slots)), DMA((2, slots))],
        cost_estimate=pl.CostEstimate(flops=10 ** 11, bytes_accessed=4 * EARLY * k_cache[0].size * 2, transcendentals=0),
        compiler_params=pltpu.CompilerParams(vmem_limit_bytes=40 * MIB),
        name='copy_early',
    )(order, k_cache, v_cache)


def qkv_kernel(own_ref, by_ref, bx_ref, bd_ref, gain_ref, w_ref, _, z_ref, hres_ref, hx_ref, wbuf, ubuf, zbuf,
               w_sem, send, recv, zsend, zrecv):
    yz, chip, core = place()
    cols = own_ref.shape[-1]
    width = z_ref.shape[-1]
    parts = ((0, COLS), (COLS, width - COLS))
    step = w_ref.shape[1] - width
    model = hx_ref.shape[-1]
    loads = []
    for n, (off, size) in enumerate(parts):
        loads.append(pltpu.make_async_copy(w_ref.at[:, lanes(core * step + off, size)],
                                           wbuf.at[:, pl.ds(off, size)], w_sem.at[n]))
        loads[-1].start()
    ynbr, partner = device(1 - yz, chip, core), device(yz, chip, 1 - core)
    far = device(1 - yz, chip, 1 - core)
    greet((ynbr, partner, far))
    copies = []
    blocks = ((own_ref, yz, chip), (by_ref, 1 - yz, chip), (bx_ref, yz, 1 - chip), (bd_ref, 1 - yz, 1 - chip))
    for k, (ref, y, ch) in enumerate(blocks):
        here = lanes((2 * (2 * ch + core) + y) * cols, cols, COLS)
        copies.append(remote(ref, hx_ref.at[:, :, here], send.at[k], recv.at[k], partner))
        copies[-1].start()
    for ref, y, ch in blocks:
        hx_ref[:, :, lanes((2 * (2 * ch + core) + y) * cols, cols, COLS)] = ref[...]
    for copy in copies:
        copy.wait_recv()

    gain = gain_ref[...].astype(jnp.float32)
    chunk = 32
    for half in range(2):
        @pl.loop(0, LANE // chunk)
        def _(r):
            hid = hx_ref[half, lanes(r * chunk, chunk, chunk), :].astype(jnp.float32)
            inv = lax.rsqrt(jnp.sum(hid * hid, axis=1, keepdims=True) / model + NORM_EPS)
            ubuf[lanes(half * LANE + r * chunk, chunk, chunk), :] = (hid * inv * gain).astype(jnp.bfloat16)

    slot = 2 * yz + core
    zcopies = []
    for n, (off, size) in enumerate(parts):
        loads[n].wait()
        z = dot(ubuf[...], wbuf[:, off:off + size]).astype(jnp.bfloat16)
        zbuf[:, :, off:off + size] = z.reshape(4, SEQS, size)
        for k, (y, co, target) in enumerate(((1 - yz, core, ynbr), (1 - yz, 1 - core, far), (yz, 1 - core, partner))):
            zcopies.append(remote(zbuf.at[2 * y + co, :, pl.ds(off, size)], z_ref.at[slot, :, pl.ds(off, size)],
                                  zsend.at[n, k], zrecv.at[n, k], target))
            zcopies[-1].start()
    z_ref[slot] = zbuf[slot]
    hres_ref[...] = hx_ref[:, :, lanes(slot_columns(yz, core), PAIR, COLS)]
    for copy in copies:
        copy.wait_send()
    for copy in zcopies:
        copy.wait()


def project_qkv(blocks, gain, w_qkv, after):
    model, half = w_qkv.shape
    width = (half // LANE + 1) // 2 * LANE
    vmem = pl.BlockSpec(memory_space=VMEM)
    anywhere = pl.BlockSpec(memory_space=pl.ANY)
    return pl.pallas_call(
        qkv_kernel,
        out_shape=(jax.ShapeDtypeStruct((4, SEQS, width), jnp.bfloat16),
                   jax.ShapeDtypeStruct((2, LANE, model // 4), jnp.bfloat16)),
        in_specs=[vmem, vmem, vmem, vmem, vmem, anywhere, anywhere],
        out_specs=(pl.BlockSpec(memory_space=VMEM), pl.BlockSpec(memory_space=VMEM)),
        scratch_shapes=[VMEM((2, LANE, model), jnp.bfloat16), VMEM((model, width), jnp.bfloat16), VMEM((ROWS, model), jnp.bfloat16),
                        VMEM((4, SEQS, width), jnp.bfloat16), TWO, FOUR, FOUR, DMA((2, 3)), DMA((2, 3))],
        compiler_params=pltpu.CompilerParams(collective_id=0, has_side_effects=True, vmem_limit_bytes=40 * MIB),
        name='qkv',
    )(*blocks, gain, w_qkv, after)


def attention_kernel(lens_ref, order_ref, z_ref, k_ref, v_ref, _, __, o_ref, ko_ref, vo_ref,
                     qs, kn, vn, os, kbuf, vbuf, sem, fsem, *, heads, group, depth, unit):
    seqs, length, dim = k_ref.shape
    tiles = (heads + 2) // 2
    split = tiles // 2
    groups = seqs // group
    sizes = length // unit

    def tile(t):
        y, local = t // tiles, t % tiles
        co = 1 if local >= split else 0
        first = (local - split * co) * dim
        return z_ref[2 * y + co, :, first:first + dim].astype(jnp.float32)

    def by_size(g, act):
        need = lens_ref[order_ref[g * group]] // unit + 1
        for size in range(1, sizes + 1):
            @pl.when(need == size)
            def _():
                act(size * unit)

    def fetch(g, rows):
        out = []
        for m in range(group):
            b = order_ref[g * group + m]
            s = lax.rem(g, depth) * group + m
            out.append(pltpu.make_async_copy(k_ref.at[b, pl.ds(0, rows)], kbuf.at[s, pl.ds(0, rows)], sem.at[0, s]))
            out.append(pltpu.make_async_copy(v_ref.at[b, pl.ds(0, rows)], vbuf.at[s, pl.ds(0, rows)], sem.at[1, s]))
        return out

    def flush(g, act):
        def tail(rows_of):
            for m in range(group):
                b = order_ref[g * group + m]
                s = lax.rem(g, depth) * group + m
                rows = rows_of(b)
                act(pltpu.make_async_copy(kbuf.at[s, rows], ko_ref.at[b, rows], fsem.at[0, s]))
                act(pltpu.make_async_copy(vbuf.at[s, rows], vo_ref.at[b, rows], fsem.at[1, s]))

        @pl.when(lax.rem(g, 4) != 2)
        def _():
            tail(lambda b: pl.ds(0, length))

        @pl.when(lax.rem(g, 4) == 2)
        def _():
            tail(lambda b: lanes(lens_ref[b] // 16 * 16, 16, 16))

    def arrive(g, begin):
        def act(rows):
            for copy in fetch(g, rows):
                if begin:
                    copy.start()
                else:
                    copy.wait()

        @pl.when(lax.rem(g, 4) != 2)
        def _():
            act(length)

        @pl.when(lax.rem(g, 4) == 2)
        def _():
            by_size(g, act)

    for g in range(2):
        arrive(jnp.int32(g), True)
    for t in range(heads):
        qs[pl.ds(t, seqs, stride=heads), :] = tile(t)
    kn[...] = tile(heads)
    vn[...] = tile(heads + 1)

    @pl.loop(0, groups)
    def _(g):
        @pl.when(g >= depth - 2)
        def _():
            flush(g - (depth - 2), lambda copy: copy.wait())

        @pl.when(g + 2 < groups)
        def _():
            arrive(g + 2, True)

        arrive(g, False)
        for m in range(group):
            b = order_ref[g * group + m]
            s = lax.rem(g, depth) * group + m
            last = lens_ref[b]
            base = pl.multiple_of(last // 16 * 16, 16)
            row = lax.broadcasted_iota(jnp.int32, (16, dim), 0) == last - base
            for buf, new in ((kbuf, kn), (vbuf, vn)):
                old = buf[s, pl.ds(base, 16), :].astype(jnp.float32)
                buf[s, pl.ds(base, 16), :] = jnp.where(row, new[pl.ds(b, 1), :], old).astype(jnp.bfloat16)

        flush(g, lambda copy: copy.start())

        def act(rows):
            scores = []
            for m in range(group):
                b = order_ref[g * group + m]
                s = lax.rem(g, depth) * group + m
                q = qs[lanes(b * heads, heads, heads), :].astype(jnp.bfloat16)
                raw = lax.dot_general(q, kbuf[s, :rows], (((1,), (1,)), ((), ())), preferred_element_type=jnp.float32)
                seen = lax.broadcasted_iota(jnp.int32, (heads, rows), 1) <= lens_ref[b]
                scores.append(jnp.where(seen, raw * dim ** -0.5, -1e30))
            tops = [jnp.max(x, axis=1, keepdims=True) for x in scores]
            probs = [jnp.exp(x - top) for x, top in zip(scores, tops)]
            sums = [1.0 / jnp.sum(x, axis=1, keepdims=True) for x in probs]
            for m in range(group):
                b = order_ref[g * group + m]
                s = lax.rem(g, depth) * group + m
                os[lanes(b * heads, heads, heads), :] = dot((probs[m] * sums[m]).astype(jnp.bfloat16), vbuf[s, :rows])

        by_size(g, act)

    for t in range(heads):
        o_ref[:, t * dim:(t + 1) * dim] = os[pl.ds(t, seqs, stride=heads), :].astype(jnp.bfloat16)

    @pl.loop(groups - (depth - 2), groups)
    def _(g):
        flush(g, lambda copy: copy.wait())


def by_length(lens):
    seqs = lens.shape[0]
    ids = jnp.arange(seqs)
    ahead = (lens[None, :] > lens[:, None]) | ((lens[None, :] == lens[:, None]) & (ids[None, :] < ids[:, None]))
    rank = jnp.sum(ahead.astype(jnp.int32), axis=1)
    late = (seqs - EARLY) // GROUP
    place_in = rank // GROUP
    place_in = jnp.where(place_in < late, place_in + (place_in + 1) // 3, 4 * (place_in - late) + 2)
    place_in = place_in * GROUP + rank % GROUP
    return jnp.sum(jnp.where(place_in[None, :] == ids[:, None], ids[None, :], 0), axis=1).astype(jnp.int32)


def attend(lens, order, z, k_cache, v_cache, k_out, v_out):
    seqs, length, dim = k_cache.shape
    heads = 32
    group, depth, unit = GROUP, DEPTH, ROWS
    anywhere = pl.BlockSpec(memory_space=pl.ANY)
    vmem = pl.BlockSpec(memory_space=VMEM)
    smem = pl.BlockSpec(memory_space=pltpu.SMEM)
    return pl.pallas_call(
        functools.partial(attention_kernel, heads=heads, group=group, depth=depth, unit=unit),
        out_shape=(jax.ShapeDtypeStruct((seqs, heads * dim), jnp.bfloat16),
                   jax.ShapeDtypeStruct(k_cache.shape, k_cache.dtype), jax.ShapeDtypeStruct(v_cache.shape, v_cache.dtype)),
        in_specs=[smem, smem, vmem, anywhere, anywhere, anywhere, anywhere],
        out_specs=(vmem, anywhere, anywhere),
        input_output_aliases={5: 1, 6: 2},
        scratch_shapes=[VMEM((seqs * heads, dim), jnp.float32), VMEM((seqs, dim), jnp.float32),
                        VMEM((seqs, dim), jnp.float32), VMEM((seqs * heads, dim), jnp.float32),
                        VMEM((group * depth, length, dim), jnp.bfloat16), VMEM((group * depth, length, dim), jnp.bfloat16),
                        DMA((2, group * depth)), DMA((2, group * depth))],
        compiler_params=pltpu.CompilerParams(vmem_limit_bytes=50 * MIB),
        name='attention',
    )(lens, order, z, k_cache, v_cache, k_out, v_out)


def mlp_kernel(o_ref, hres, gain_ref, wo_ref, gu_ref, wd_ref, out_ref,
               og, wo, ys, yr, own, h1, inv_ref, ubuf, ue, gub, gacc, mbuf, wd, ps, pr, acc, fs, fr, xs, st,
               s_wo, s_gu, s_wd, send, recv, ysend, yrecv, hsend, hrecv, asend, arecv, osend, orecv, ssend, srecv,
               psend, precv, fsend, frecv, xsend, xrecv):
    yz, chip, core = place()
    half = wo_ref.shape[0]
    model = wo_ref.shape[1]
    inner = gu_ref.shape[2] // 2
    tiles = inner // COLS
    ynbr, xnbr, partner = device(1 - yz, chip, core), device(yz, 1 - chip, core), device(yz, chip, 1 - core)
    far = device(1 - yz, chip, 1 - core)

    wo_copies = [pltpu.make_async_copy(wo_ref.at[:, lanes(core * half + n * COLS, COLS, COLS)], wo.at[n], s_wo.at[n])
                 for n in range(4)]

    def place_of(p):
        y = jnp.where(p < 4, yz, 1 - yz)
        return (p % 4) // 2 * 4 + 2 * y + p % 2

    def gu_copies(q):
        s = lax.rem(q, 3)
        n = lax.rem(q, tiles)
        return [pltpu.make_async_copy(
            gu_ref.at[lanes(place_of(q // tiles * 4 + r) * COLS, COLS, COLS), :, lanes(core * inner + n * COLS, COLS, COLS)],
            gub.at[s, pl.ds(r * COLS, COLS)], s_gu.at[s, r]) for r in range(4)]

    def column(t):
        k = t // 2
        y = jnp.where(k < 2, 1 - yz, yz)
        ch = jnp.where(k % 2 == 0, 1 - chip, chip)
        co = jnp.where(t % 2 == 0, 1 - core, core)
        return 2 * (2 * ch + co) + y

    def wd_copies(t):
        s = lax.rem(t, 3)
        rows = inner // 2
        return [pltpu.make_async_copy(wd_ref.at[lanes(core * inner + r * rows, rows, rows), lanes(column(t) * COLS, COLS, COLS)],
                                      wd.at[s, pl.ds(r * rows, rows)], s_wd.at[s, r]) for r in range(2)]

    for copy in wo_copies:
        copy.start()
    greet((ynbr, xnbr, partner, far))

    slot = 2 * yz + core
    to_y = remote(o_ref.at[:, lanes((1 - yz) * half, half, COLS)], og.at[slot], send.at[0], recv.at[0], ynbr)
    to_y.start()
    to_p = remote(o_ref.at[:, lanes(yz * half, half, COLS)], og.at[slot], send.at[1], recv.at[1], partner)
    to_p.start()
    og[slot] = o_ref[:, lanes(yz * half, half, COLS)]
    for q in range(3):
        for copy in gu_copies(jnp.int32(q)):
            copy.start()
    for t in range(3):
        for copy in wd_copies(jnp.int32(t)):
            copy.start()
    for copy in wo_copies:
        copy.wait()
    to_y.wait_recv()
    theirs = og.at[2 * (1 - yz) + core]
    onward = remote(theirs, theirs, send.at[2], recv.at[2], partner)
    onward.start()
    to_p.wait_recv()
    onward.wait_recv()

    def y_copy(e):
        return remote(ys.at[e], yr.at[e], ysend.at[e], yrecv.at[e], ynbr)

    @pl.loop(0, 2)
    def _(e):
        ys[e] = dot(og[...].reshape(ROWS, half), wo[2 * (1 - yz) + e]).astype(jnp.bfloat16)
        y_copy(e).start()

    @pl.loop(0, 2)
    def _(e):
        own[e] = dot(og[...].reshape(ROWS, half), wo[2 * yz + e])

    first = 4 * core + 2 * yz

    def h_send(e):
        return remote(h1.at[first + e], h1.at[first + e], hsend.at[e], hrecv.at[e], partner)

    def a_send(e):
        return remote(h1.at[first + e], h1.at[first + e], asend.at[e], arecv.at[e], ynbr)

    def onto(e):
        there = h1.at[4 * core + 2 * (1 - yz) + e]
        return remote(there, there, osend.at[e], orecv.at[e], partner)

    power = jnp.zeros((ROWS, 1), jnp.float32)
    for e in range(2):
        y_copy(e).wait_recv()
        res = hres[:, :, e * COLS:(e + 1) * COLS].reshape(ROWS, COLS).astype(jnp.float32)
        hid = (res + (own[e] + yr[e].astype(jnp.float32))).astype(jnp.bfloat16)
        h1[first + e] = hid
        h_send(e).start()
        hid = hid.astype(jnp.float32)
        power += jnp.sum(hid * hid, axis=1, keepdims=True)

    at_lane = lax.broadcasted_iota(jnp.int32, (32, 8, LANE), 2) == lax.broadcasted_iota(jnp.int32, (32, 8, LANE), 0)
    st[slot] = jnp.sum(jnp.where(at_lane, power.reshape(32, 8, 1), 0.0), axis=0)
    stats = [remote(st.at[slot], st.at[slot], ssend.at[k], srecv.at[k], target)
             for k, target in enumerate((ynbr, far, partner))]
    for copy in stats:
        copy.start()
    for e in range(2):
        a_send(e).start()
    for copy in stats:
        copy.wait_recv()
    total = (st[0] + st[1]) + (st[2] + st[3])
    power = jnp.sum(jnp.where(at_lane, total[None], 0.0), axis=2, keepdims=True).reshape(ROWS, 1)
    inv_ref[...] = jnp.broadcast_to(lax.rsqrt(power / model + NORM_EPS), (ROWS, LANE))

    at = lax.broadcasted_iota(jnp.int32, (LANE, COLS), 1)
    spread = (at % ROWS == 2 * lax.broadcasted_iota(jnp.int32, (LANE, COLS), 0) + at // ROWS).astype(jnp.bfloat16)

    def prepare(p):
        b = place_of(p)
        gain = gain_ref[:, lanes(b * COLS, COLS, COLS)].astype(jnp.float32)
        ubuf[...] = (h1[b].astype(jnp.float32) * inv_ref[:, :1] * gain).astype(jnp.bfloat16)
        for q in range(4):
            wide = dot(ubuf[:, q * LANE:(q + 1) * LANE], spread).astype(jnp.bfloat16)
            ue[:ROWS, lanes(p * PAIR + q * ROWS, ROWS, ROWS)] = wide[:, :ROWS]
            ue[ROWS:, lanes(p * PAIR + q * ROWS, ROWS, ROWS)] = wide[:, ROWS:]

    for e in range(2):
        h_send(e).wait_recv()

    @pl.loop(0, 4)
    def _(p):
        prepare(p)

    def more(q):
        @pl.when(q + 3 < 2 * tiles)
        def _():
            for copy in gu_copies(q + 3):
                copy.start()

    @pl.loop(0, tiles)
    def _(n):
        @pl.when((n == 2) | (n == 4))
        def _():
            a_send(n // 2 - 1).wait_recv()
            onto(n // 2 - 1).start()

        for copy in gu_copies(n):
            copy.wait()
        gacc[n] = dot(ue[:, :model], gub.at[lax.rem(n, 3)].reshape(model, COLS)[...])
        more(n)

    for e in range(2):
        onto(e).wait_recv()

    @pl.loop(4, 8)
    def _(p):
        prepare(p)

    @pl.loop(0, tiles)
    def _(n):
        q = n + tiles
        for copy in gu_copies(q):
            copy.wait()
        both = gacc[n] + dot(ue[:, model:], gub.at[lax.rem(q, 3)].reshape(model, COLS)[...])
        more(q)
        gate = both[:ROWS].astype(jnp.bfloat16).astype(jnp.float32)
        up = both[ROWS:].astype(jnp.bfloat16).astype(jnp.float32)
        mbuf[:, lanes(n * COLS, COLS, COLS)] = (gate * jax.nn.sigmoid(gate) * up).astype(jnp.bfloat16)

    def p_copy(k):
        return remote(ps.at[k], pr.at[k], psend.at[k], precv.at[k], partner)

    def f_copy(k):
        return remote(fs.at[k], fr.at[k], fsend.at[k], frecv.at[k], ynbr)

    x_copy = remote(xs, out_ref.at[:, chip], xsend.at[0], xrecv.at[0], xnbr)

    @pl.loop(0, 4)
    def _(k):
        for side in range(2):
            t = 2 * k + side
            s = lax.rem(t, 3)
            for copy in wd_copies(t):
                copy.wait()
            part = dot(mbuf[...], wd[s])

            @pl.when(t + 3 < 8)
            def _():
                for copy in wd_copies(t + 3):
                    copy.start()

            if side == 0:
                ps[k] = part.astype(jnp.bfloat16)
                p_copy(k).start()
            else:
                acc[...] = part
        p_copy(k).wait_recv()
        acc[...] += pr[k].astype(jnp.float32)

        @pl.when(k < 2)
        def _():
            fs[k] = acc[...].astype(jnp.bfloat16)
            f_copy(k).start()

        @pl.when(k >= 2)
        def _():
            f_copy(k - 2).wait_recv()
            total = acc[...] + fr[k - 2].astype(jnp.float32)
            final = (h1[column(2 * k + 1)].astype(jnp.float32) + total).astype(jnp.bfloat16).reshape(2, LANE, COLS)

            @pl.when(k == 2)
            def _():
                xs[...] = final
                x_copy.start()

            @pl.when(k == 3)
            def _():
                out_ref[:, chip] = final

    x_copy.wait()
    for copy in (to_y, to_p, onward):
        copy.wait_send()

    for copy in stats:
        copy.wait_send()
    for n in range(4):
        p_copy(n).wait_send()
    for n in range(2):
        for copy in (y_copy(n), h_send(n), a_send(n), onto(n), f_copy(n)):
            copy.wait_send()


def mlp(o, hres, gain, w_out, w_gate_up, w_down):
    half, model = w_out.shape
    inner = w_gate_up.shape[2] // 2
    anywhere = pl.BlockSpec(memory_space=pl.ANY)
    vmem = pl.BlockSpec(memory_space=VMEM)
    bf16 = jnp.bfloat16
    out = pl.pallas_call(
        mlp_kernel,
        out_shape=jax.ShapeDtypeStruct((2, 2, LANE, COLS), bf16),
        in_specs=[vmem, vmem, vmem, anywhere, anywhere, anywhere],
        out_specs=vmem,
        scratch_shapes=[
            VMEM((4, SEQS, half), bf16), VMEM((4, half, COLS), bf16),
            *(VMEM((2, ROWS, COLS), bf16),) * 2, VMEM((2, ROWS, COLS), jnp.float32), VMEM((8, ROWS, COLS), bf16),
            VMEM((ROWS, LANE), jnp.float32), VMEM((ROWS, COLS), bf16), VMEM((COLS, 2 * model), bf16),
            VMEM((3, half, 2, COLS), bf16), VMEM((inner // COLS, COLS, COLS), jnp.float32),
            VMEM((ROWS, inner), bf16), VMEM((3, inner, COLS), bf16),
            *(VMEM((4, ROWS, COLS), bf16),) * 2, VMEM((ROWS, COLS), jnp.float32),
            *(VMEM((2, ROWS, COLS), bf16),) * 2, VMEM((2, LANE, COLS), bf16), VMEM((4, 8, LANE), jnp.float32),
            FOUR, DMA((3, 4)), DMA((3, 2)),
            THREE, THREE, TWO, TWO, TWO, TWO, TWO, TWO, TWO, TWO,
            THREE, THREE,
            FOUR, FOUR, TWO, TWO, ONE, ONE,
        ],
        compiler_params=pltpu.CompilerParams(collective_id=1, has_side_effects=True, vmem_limit_bytes=60 * MIB),
        name='mlp',
    )(o, hres, gain, w_out, w_gate_up, w_down)
    return out.reshape(COLS, COLS)


def move_kernel(h_ref, out_ref, sem):
    copy = pltpu.make_async_copy(h_ref, out_ref, sem)
    copy.start()
    copy.wait()


def move(hidden):
    return pl.pallas_call(
        move_kernel,
        out_shape=jax.ShapeDtypeStruct(hidden.shape, hidden.dtype),
        in_specs=[pl.BlockSpec(memory_space=VMEM)],
        out_specs=pl.BlockSpec(memory_space=pl.ANY),
        scratch_shapes=[DMA],
        name='move',
    )(hidden)


def solution(mesh):
    batch_axes = ('replica', 'yz', 'x')
    hidden_spec = P('replica', ('x', 'yz'))
    cache_spec = P(None, batch_axes, None, None)

    def local_step(hidden, seq_lens, attn_gain, mlp_gain, w_qkv, w_out, w_gate_up, w_down, k_cache, v_cache):
        k_layers = []
        v_layers = []
        for layer in range(w_qkv.shape[0]):
            order = by_length(seq_lens)
            rows = hidden.reshape(2, 2, LANE, hidden.shape[1])
            chip = lax.axis_index('x') // 2
            own = lax.dynamic_index_in_dim(rows, chip, 1, keepdims=False)
            other = lax.dynamic_index_in_dim(rows, 1 - chip, 1, keepdims=False)
            by = lax.ppermute(own, 'yz', [(0, 1), (1, 0)])
            bx = lax.ppermute(other, 'x', [(j, j ^ 2) for j in range(4)])
            bd = lax.ppermute(other, ('yz', 'x'), [(j, j ^ 6) for j in range(8)])
            k_upd, v_upd = copy_early(order, k_cache[layer], v_cache[layer])
            z, hres = project_qkv((own, by, bx, bd), attn_gain[layer:layer + 1], w_qkv[layer], k_upd)
            o, k_upd, v_upd = attend(seq_lens, order, z, k_cache[layer], v_cache[layer], k_upd, v_upd)
            k_layers.append(k_upd)
            v_layers.append(v_upd)
            hidden = mlp(o, hres, mlp_gain[layer:layer + 1], w_out[layer], w_gate_up[layer], w_down[layer])
        return move(hidden), jnp.stack(k_layers), jnp.stack(v_layers)

    return jax.shard_map(
        local_step,
        mesh=mesh,
        in_specs=(hidden_spec, P(batch_axes), P(None, None), P(None, None), P(None, None, 'yz'), P(None, 'yz', None),
                  P(None, None, None, 'yz'), P(None, 'yz', None), cache_spec, cache_spec),
        out_specs=(hidden_spec, cache_spec, cache_spec),
        check_vma=False)
```
